256 devices in a mesh: angle: 2 (over y_hi), ty: 16 (over z, core), tx: 8 (over x, y_lo).
Axes of the slice: x: 4, y: 4 (y_hi: 2, y_lo: 2; y = y_hi * 2 + y_lo), z: 8, core: 2. Of those that a mesh axis runs over, the one named last changes fastest.
Arguments:
- object_slices: float32 [2, 2, 4096, 8192], P('angle', None, 'ty', 'tx'), may hold values from -5 to 5
- probe_field: float32 [2, 256, 256], replicated, may hold values from -6 to 6
- positions: int32 [2, 16, 8, 4, 2], P('angle', 'ty', 'tx'), may hold values from 0 to 7936, as said below
- live_slots: int32 [2, 16, 8], P('angle', 'ty', 'tx'), may hold values from 1 to 4, as said below
- photon_counts: int32 [2, 16, 8, 4, 256, 256], P('angle', 'ty', 'tx'), may hold values from 1 to 1600
Outputs:
- new_object: float32 [2, 2, 4096, 8192], P('angle', None, 'ty', 'tx')
- new_probe: float32 [2, 256, 256], P(None, 'ty')
The draws below stay inside these ranges and needn't reach their ends.
Inputs may be any that keep to these rules, and one draw needn't show every extreme that they name: `positions`: A slot's patch lies inside the object and its centre (top-left plus 128) lies in the rows and columns of the tile that holds the slot: rows r * 256 to (r + 1) * 256 - 1, columns c * 1024 to (c + 1) * 1024 - 1. `live_slots`: some tile of every draw uses all 4 slots.
All inputs are finite; a program needn't handle non-finite values.
Results may differ from the reference program's by a relative error of at most 0.0003.
Values sent between devices are 32-bit elements; how exact they have to be, the bound alone decides.
A program may use at most 128 MiB of HBM per device.

```python
import jax
import jax.numpy as jnp
from jax import lax

P_SIZE = 256
TR = 256
TC = 1024
SLOTS = 4
ANGLES = 2
NR = 4096
NC = 8192
N_TY = 16
N_TX = 8


def draw_positions(key, part):
    shape = (ANGLES, N_TY, N_TX, SLOTS)
    first_key, second_key = jax.random.split(jax.random.fold_in(key, 11))
    row_draw = jax.random.randint(first_key, shape, 0, TR)
    col_draw = jax.random.randint(second_key, shape, 0, TC)
    tile_row = lax.broadcasted_iota(jnp.int32, shape, 1)
    tile_col = lax.broadcasted_iota(jnp.int32, shape, 2)
    row_start = jnp.clip(tile_row * TR - P_SIZE // 2 + row_draw, 0, NR - P_SIZE)
    col_start = jnp.clip(tile_col * TC - P_SIZE // 2 + col_draw, 0, NC - P_SIZE)
    return jnp.stack([row_start, col_start], axis=-1).astype(jnp.int32)


def draw_live_slots(key, part):
    shape = (ANGLES, N_TY, N_TX)
    first_key, second_key, third_key = jax.random.split(jax.random.fold_in(key, 23), 3)
    sparse = jax.random.randint(first_key, shape, 1, max(SLOTS // 4, 1) + 1)
    dense = jax.random.randint(second_key, shape, 0, 8) == 0
    values = jnp.where(dense, SLOTS, sparse).reshape(-1)
    chosen = jax.random.randint(third_key, (), 0, ANGLES * N_TY * N_TX)
    values = jnp.where(jnp.arange(ANGLES * N_TY * N_TX) == chosen, SLOTS, values)
    return values.reshape(shape).astype(jnp.int32)


def set_ends(result, own_key, smallest, high):
    longest = result.shape.index(max(result.shape))
    spots = []
    for shift in (0, 1):
        where = [jax.random.randint(jax.random.fold_in(own_key, axis), (), 0, length) for axis, length in enumerate(result.shape)]
        where[longest] = (where[longest] + shift) % result.shape[longest]
        spots.append(tuple(where))
    return result.at[spots[0]].set(smallest).at[spots[1]].set(high)


def block_scale(stream_key, shape, cuts, smallest, largest):
    level, own = 1.0, jax.random.fold_in(stream_key, 6)
    for axis_at, parts in cuts:
        draws = jnp.exp(jax.random.uniform(jax.random.fold_in(own, axis_at), (parts,), jnp.float32, smallest / len(cuts), largest / len(cuts)))
        level = level * jnp.repeat(draws, shape[axis_at] // parts).reshape([-1 if axis == axis_at else 1 for axis in range(len(shape))])
    return level


def noise(stream_key, extent, width, limit, pieces=(), kind=jnp.bfloat16):
    gain = block_scale(stream_key, extent, pieces, -0.22, 0.18) if pieces else 1.0
    values = jax.random.normal(stream_key, extent, jnp.float32) * width * gain
    return jnp.minimum(jnp.maximum(values, -limit), limit).astype(kind)


def setup_inputs(seed: int = 0) -> dict:
    key_of = jax.random.split(jax.random.key(seed), 6)
    object_slices = noise(key_of[0], (ANGLES, 2, NR, NC), 0.7, 5.0, ((0, 2), (2, 16), (3, 8)), jnp.float32)
    probe_field = noise(key_of[1], (2, P_SIZE, P_SIZE), 1.0, 6.0, (), jnp.float32)
    positions = draw_positions(jax.random.fold_in(key_of[5], 71), 0)
    live_slots = draw_live_slots(jax.random.fold_in(key_of[5], 71), 0)
    photon_counts = set_ends(jax.random.randint(key_of[4], (ANGLES, N_TY, N_TX, SLOTS, P_SIZE, P_SIZE), 1, 1601), jax.random.fold_in(key_of[4], 1), 1, 1600).astype(jnp.int32)
    return {"object_slices": object_slices, "probe_field": probe_field, "positions": positions, "live_slots": live_slots, "photon_counts": photon_counts}


def reference(object_slices, probe_field, positions, live_slots, photon_counts):
    ftype = object_slices.dtype
    probe_wave = lax.complex(probe_field[0], probe_field[1])
    probe_power = probe_field[0] * probe_field[0] + probe_field[1] * probe_field[1]
    slot_index = jnp.arange(SLOTS, dtype=jnp.int32)
    probe_num = jnp.zeros((P_SIZE, P_SIZE), probe_wave.dtype)
    probe_den = jnp.zeros((P_SIZE, P_SIZE), ftype)
    numerators = []
    denominators = []
    fields = []
    for angle_index in range(ANGLES):
        field = lax.complex(object_slices[angle_index, 0], object_slices[angle_index, 1])
        spots = positions[angle_index].reshape(-1, 2).astype(jnp.int32)
        weights = (slot_index[None, None, :] < live_slots[angle_index][:, :, None]).astype(ftype).reshape(-1)
        measured = photon_counts[angle_index].reshape(-1, P_SIZE, P_SIZE)

        def deposit(carry, item):
            obj_num, obj_den, pr_num, pr_den = carry
            spot, weight, count = item
            row_at = spot[0].astype(jnp.int32)
            col_at = spot[1].astype(jnp.int32)
            patch = lax.dynamic_slice(field, (row_at, col_at), (P_SIZE, P_SIZE))
            wave = probe_wave * patch
            far = jnp.fft.fft2(wave, norm='ortho')
            amplitude = 0.05 * jnp.sqrt(count.astype(ftype))
            factor = amplitude * lax.rsqrt(jnp.maximum(far.real * far.real + far.imag * far.imag, 0.0625))
            gap = (jnp.fft.ifft2(far * factor, norm='ortho') - wave) * weight
            current = lax.dynamic_slice(obj_num, (row_at, col_at), (P_SIZE, P_SIZE))
            obj_num = lax.dynamic_update_slice(obj_num, current + jnp.conj(probe_wave) * gap, (row_at, col_at))
            current_den = lax.dynamic_slice(obj_den, (row_at, col_at), (P_SIZE, P_SIZE))
            obj_den = lax.dynamic_update_slice(obj_den, current_den + weight * probe_power, (row_at, col_at))
            pr_num = pr_num + jnp.conj(patch) * gap
            pr_den = pr_den + weight * (patch.real * patch.real + patch.imag * patch.imag)
            return ((obj_num, obj_den, pr_num, pr_den), None)
        start = (jnp.zeros(field.shape, field.dtype), jnp.zeros(field.shape, ftype), probe_num, probe_den)
        (obj_num, obj_den, probe_num, probe_den), _ = lax.scan(deposit, start, (spots, weights, measured))
        numerators.append(obj_num)
        denominators.append(obj_den)
        fields.append(field)
    peak_obj = jnp.max(jnp.stack([jnp.max(den) for den in denominators]))
    peak_probe = jnp.max(probe_den)
    updated = []
    for angle_index in range(ANGLES):
        value = fields[angle_index] + numerators[angle_index] / (denominators[angle_index] + 0.1 * peak_obj)
        updated.append(jnp.stack([value.real, value.imag]))
    new_object = jnp.stack(updated)
    probe_new = probe_wave + probe_num / (probe_den + 0.1 * peak_probe)
    new_probe = jnp.stack([probe_new.real, probe_new.imag])
    return (new_object, new_probe)
```

```python
import functools
import math

import jax
import jax.numpy as jnp
import numpy as np
from jax import lax
from jax.experimental import pallas as pl
from jax.experimental.pallas import tpu as pltpu
from jax.sharding import PartitionSpec as P

MESH = pl.DeviceIdType.MESH
F32 = jnp.float32
BF16 = jnp.bfloat16
SIZE = 256
HALF = 128
TR = 256
TC = 1024
WR = TR + SIZE
WC = TC + SIZE
N_TY = 16
N_TX = 8
N_ANGLE = 2
N_XY = N_ANGLE * N_TX


def tables():
    n = np.arange(HALF)
    base = np.exp(-2j * np.pi * np.outer(n, n) / HALF) / 16.0
    odd = base * np.exp(-2j * np.pi * n / SIZE)[None, :]

    def real_form(m):
        return np.block([[m.real, -m.imag], [m.imag, m.real]])

    mats = [real_form(base), real_form(odd)]
    mats = np.stack([mats[0], mats[1], mats[0].T, mats[1].T]).astype(np.float32)
    high = mats.astype(jnp.bfloat16)
    low = (mats - high.astype(np.float32)).astype(jnp.bfloat16)
    order = np.zeros((SIZE, SIZE), np.float32)
    for j in range(SIZE):
        order[2 * j if j < HALF else 2 * (j - HALF) + 1, j] = 1.0
    both = np.stack([order, order.T]).astype(jnp.bfloat16)
    return high, low, both


TABLE_HIGH, TABLE_LOW, TABLE_ORDER = tables()


def remote(src, dst, send, recv, **where):
    return pltpu.make_async_remote_copy(
        src_ref=src, dst_ref=dst, send_sem=send, recv_sem=recv, device_id=where, device_id_type=MESH
    )


def halo_kernel(tile, meta, wide, around, hs, hr, vs, vr, cs, cr, ms, mr, local):
    ty, tx = lax.axis_index("ty"), lax.axis_index("tx")
    up, down = lax.rem(ty + N_TY - 1, N_TY), lax.rem(ty + 1, N_TY)
    left, right = lax.rem(tx + N_TX - 1, N_TX), lax.rem(tx + 1, N_TX)
    barrier = pltpu.get_barrier_semaphore()
    for where in ({"ty": up}, {"ty": down}, {"tx": left}, {"tx": right}):
        pl.semaphore_signal(barrier, inc=1, device_id=where, device_id_type=MESH)
    middle = pltpu.make_async_copy(
        tile, wide.at[:, pl.ds(HALF, TR), pl.ds(HALF, TC)], local.at[0]
    )
    middle.start()
    own = pltpu.make_async_copy(meta, around.at[1, 1], local.at[1])
    own.start()
    pl.semaphore_wait(barrier, 4)
    rows = pl.ds(HALF, TR)
    sides = [
        remote(tile.at[:, :, pl.ds(0, HALF)], wide.at[:, rows, pl.ds(HALF + TC, HALF)], hs.at[0], hr.at[0], tx=left),
        remote(tile.at[:, :, pl.ds(TC - HALF, HALF)], wide.at[:, rows, pl.ds(0, HALF)], hs.at[1], hr.at[1], tx=right),
        remote(meta, around.at[1, 2], ms.at[0], mr.at[0], tx=left),
        remote(meta, around.at[1, 0], ms.at[1], mr.at[1], tx=right),
    ]
    cols = pl.ds(HALF, TC)
    ends = [
        remote(tile.at[:, pl.ds(0, HALF), :], wide.at[:, pl.ds(HALF + TR, HALF), cols], vs.at[0], vr.at[0], ty=up),
        remote(tile.at[:, pl.ds(TR - HALF, HALF), :], wide.at[:, pl.ds(0, HALF), cols], vs.at[1], vr.at[1], ty=down),
    ]
    sides[2].start()
    sides[3].start()
    sides[0].start()
    sides[1].start()
    ends[0].start()
    ends[1].start()
    own.wait()
    sides[2].wait()
    sides[3].wait()
    lines = [
        remote(around.at[1], around.at[2], ms.at[2], mr.at[2], ty=up),
        remote(around.at[1], around.at[0], ms.at[3], mr.at[3], ty=down),
    ]
    for line in lines:
        line.start()
    corners = []
    for side, strip in ((1, pl.ds(0, HALF)), (0, pl.ds(HALF + TC, HALF))):
        sides[side].wait_recv()
        for way, (src, dst, where) in enumerate(
            ((HALF, HALF + TR, {"ty": up}), (TR, 0, {"ty": down}))
        ):
            at = 2 * side + way
            corner = remote(
                wide.at[:, pl.ds(src, HALF), strip], wide.at[:, pl.ds(dst, HALF), strip], cs.at[at], cr.at[at], **where
            )
            corner.start()
            corners.append(corner)
    middle.wait()
    sides[0].wait_send()
    sides[1].wait_send()
    for copy in ends + lines + corners:
        copy.wait()


def split(x):
    high = x.astype(BF16)
    return high, (x - high.astype(F32)).astype(BF16)


def dot(a, b):
    return jnp.dot(a, b, preferred_element_type=F32)


def patch_kernel(
    around_s, wide, probe, counts, high, low, order, canvas, sums, den_out, peak_out, den, pad
):
    f32 = F32
    ty, tx = lax.axis_index("ty"), lax.axis_index("tx")
    canvas[...] = jnp.zeros_like(canvas)
    sums[...] = jnp.zeros_like(sums)
    lane33 = lax.broadcasted_iota(jnp.int32, (33, 8, HALF), 2)
    sub32 = lax.broadcasted_iota(jnp.int32, (32, 8, HALF), 1)
    sub33 = lax.broadcasted_iota(jnp.int32, (33, 8, HALF), 1)
    lane32 = lax.broadcasted_iota(jnp.int32, (32, 8, HALF), 2)
    blank = jnp.zeros((1, 8, HALF), f32)

    def place(ref, row, col, x):
        at_row, by_row = pl.multiple_of(row // 8 * 8, 8), lax.rem(row, 8)
        at_col, by_col = pl.multiple_of(col // HALF * HALF, HALF), lax.rem(col, HALF)

        def turned(part):
            y = pltpu.roll(part.reshape(32, 8, HALF), by_col, 2)
            y = pltpu.roll(y, by_row, 1)
            return y

        one, two = turned(x[:, :HALF]), turned(x[:, HALF:])
        inside = lane32 >= by_col
        below = sub33 >= by_row
        zero = jnp.zeros_like(one)
        for step, part in enumerate(
            (jnp.where(inside, one, zero), jnp.where(inside, two, one), jnp.where(inside, zero, two))
        ):
            moved = jnp.where(
                below, jnp.concatenate([part, blank], 0), jnp.concatenate([blank, part], 0)
            )
            rows, cols = pl.ds(at_row, 264), pl.ds(at_col + HALF * step, HALF)
            ref[rows, cols] += moved.reshape(264, HALF)

    def cut(ref, row, col):
        at_row, by_row = pl.multiple_of(row // 8 * 8, 8), lax.rem(row, 8)
        at_col, by_col = pl.multiple_of(col // HALF * HALF, HALF), lax.rem(col, HALF)
        back_row, back_col = lax.rem(8 - by_row, 8), lax.rem(HALF - by_col, HALF)
        parts = []
        for step in range(3):
            x = ref[pl.ds(at_row, 264), pl.ds(at_col + HALF * step, HALF)].reshape(33, 8, HALF)
            parts.append(pltpu.roll(x, back_col, 2))
        done = []
        for step in range(2):
            x = jnp.where(lane33 < HALF - by_col, parts[step], parts[step + 1])
            x = pltpu.roll(x, back_row, 1)
            x = jnp.where(sub32 < 8 - by_row, x[:32], x[1:])
            done.append(x.reshape(SIZE, HALF))
        return jnp.concatenate(done, 1)

    def from_left(which, x):
        a, b = split(x)
        return dot(high[which], a) + (dot(high[which], b) + dot(low[which], a))

    def from_right(x, which):
        a, b = split(x)
        return dot(a, high[which]) + (dot(b, high[which]) + dot(a, low[which]))

    qr, qi = probe[0], probe[1]
    power = qr * qr + qi * qi
    live = around_s[1, 1, 0, 8]

    def one_slot(slot, carry):
        row = around_s[1, 1, 0, 2 * slot] - (ty * TR - HALF)
        col = around_s[1, 1, 0, 2 * slot + 1] - (tx * TC - HALF)
        xr, xi = cut(wide.at[0], row, col), cut(wide.at[1], row, col)
        qr, qi = probe[0], probe[1]
        pr, pi = qr * xr - qi * xi, qr * xi + qi * xr
        even = from_right(
            jnp.concatenate([pr[:, :HALF] + pr[:, HALF:], pi[:, :HALF] + pi[:, HALF:]], 1), 2
        )
        odd = from_right(
            jnp.concatenate([pr[:, :HALF] - pr[:, HALF:], pi[:, :HALF] - pi[:, HALF:]], 1), 3
        )
        mr = jnp.concatenate([even[:, :HALF], odd[:, :HALF]], 1)
        mi = jnp.concatenate([even[:, HALF:], odd[:, HALF:]], 1)
        fe = from_left(0, jnp.concatenate([mr[:HALF] + mr[HALF:], mi[:HALF] + mi[HALF:]], 0))
        fo = from_left(1, jnp.concatenate([mr[:HALF] - mr[HALF:], mi[:HALF] - mi[HALF:]], 0))
        count = counts[slot]
        tens = lax.shift_right_logical(count, 4)
        ones = count - 16 * tens
        tens = dot(dot(order[1], tens.astype(F32).astype(BF16)).astype(BF16), order[0])
        ones = dot(dot(order[1], ones.astype(F32).astype(BF16)).astype(BF16), order[0])
        count = 16.0 * tens + ones

        def scaled(f, c):
            re, im = f[:HALF], f[HALF:]
            size = jnp.maximum(re * re + im * im, 0.0625)
            factor = (0.05 * c) * lax.rsqrt(c * size)
            return jnp.concatenate([re * factor, im * factor], 0)

        ge = from_left(2, scaled(fe, count[:HALF]))
        go = from_left(3, scaled(fo, count[HALF:]))
        top, bottom = ge + go, ge - go
        hr_ = jnp.concatenate([top[:HALF], bottom[:HALF]], 0)
        hi_ = jnp.concatenate([top[HALF:], bottom[HALF:]], 0)
        be = from_right(jnp.concatenate([hr_[:, :HALF], hi_[:, :HALF]], 1), 0)
        bo = from_right(jnp.concatenate([hr_[:, HALF:], hi_[:, HALF:]], 1), 1)
        first, second = be + bo, be - bo
        dr = jnp.concatenate([first[:, :HALF], second[:, :HALF]], 1) - pr
        di = jnp.concatenate([first[:, HALF:], second[:, HALF:]], 1) - pi
        place(canvas.at[0], row, col, qr * dr + qi * di)
        place(canvas.at[1], row, col, qr * di - qi * dr)
        add = (xr * dr + xi * di, xr * di - xi * dr, xr * xr + xi * xi)
        for channel in range(3):
            x = add[channel].reshape(8, 2, 2, 8, SIZE)
            for parity in range(2):
                y = x[:, parity].reshape(16, 8, SIZE)
                sums[parity, :, channel] += y
        return carry

    lax.fori_loop(0, live, one_slot, 0)

    den[pl.ds(SIZE, TR), pl.ds(SIZE, TC)] = jnp.zeros((TR, TC), f32)
    pad[...] = power

    def one_place(item, carry):
        up_by, rest = item // 12, lax.rem(item, 12)
        left_by, slot = rest // 4, lax.rem(rest, 4)
        row = around_s[up_by, left_by, 0, 2 * slot] - ty * TR
        col = around_s[up_by, left_by, 0, 2 * slot + 1] - tx * TC
        used = slot < around_s[up_by, left_by, 0, 8]
        near = (row > -SIZE) & (row < TR) & (col > -SIZE) & (col < TC)

        @pl.when(used & near)
        def _():
            place(den, row + SIZE, col + SIZE, pad[...])

        return carry

    lax.fori_loop(0, 36, one_place, 0)
    total = den[pl.ds(SIZE, TR), pl.ds(SIZE, TC)]
    den_out[...] = total
    peak_out[...] = jnp.broadcast_to(jnp.max(total), (8, HALF))


def return_kernel(
    canvas, sums, peak_in, folded, psum, peaks,
    pair, mine, box, part, zbox, whole, final, pk, pkxy, pkty, vin, cin, hin, hout,
    vs, vr, cs, cr, hs, hr, ds_, dr_, xs, xr, zs, zr, bs, br, qs, qr, ts, tr,
):
    angle, ty, tx = lax.axis_index("angle"), lax.axis_index("ty"), lax.axis_index("tx")
    up, down = lax.rem(ty + N_TY - 1, N_TY), lax.rem(ty + 1, N_TY)
    left, right = lax.rem(tx + N_TX - 1, N_TX), lax.rem(tx + 1, N_TX)
    me = angle * N_TX + tx
    core, z = lax.rem(ty, 2), ty // 2
    barrier = pltpu.get_barrier_semaphore()

    def xy_peer(step):
        other = lax.rem(me + step, N_XY)
        return other, {"angle": other // N_TX, "tx": lax.rem(other, N_TX)}

    def ty_peer(step):
        other = lax.rem(ty + step, N_TY)
        return other, {"ty": other}

    for step in range(1, 16):
        pl.semaphore_signal(barrier, inc=1, device_id=xy_peer(step)[1], device_id_type=MESH)
        pl.semaphore_signal(barrier, inc=1, device_id=ty_peer(step)[1], device_id_type=MESH)
    pl.semaphore_wait(barrier, 30)

    corners = []
    for side, strip in ((0, pl.ds(0, HALF)), (1, pl.ds(HALF + TC, HALF))):
        for way, (src, where) in enumerate(((0, {"ty": up}), (HALF + TR, {"ty": down}))):
            at = 2 * side + way
            corners.append(
                remote(canvas.at[:, pl.ds(src, HALF), strip], cin.at[at], cs.at[at], cr.at[at], **where)
            )
            corners[-1].start()
    with_pair = remote(sums.at[1 - core], pair, ds_.at[0], dr_.at[0], ty=ty + 1 - 2 * core)
    with_pair.start()
    cols = pl.ds(HALF, TC)
    ends = [
        remote(canvas.at[:, pl.ds(0, HALF), cols], vin.at[0], vs.at[0], vr.at[0], ty=up),
        remote(canvas.at[:, pl.ds(HALF + TR, HALF), cols], vin.at[1], vs.at[1], vr.at[1], ty=down),
    ]
    for copy in ends:
        copy.start()
    sent = []
    for step in range(1, 16):
        other, where = xy_peer(step)
        copy = remote(peak_in, pkxy.at[step], qs.at[step], qr.at[step], **where)
        copy.start()
        sent.append(copy)

    with_pair.wait()
    mine[...] = sums[core] + pair[...]
    spread = []
    for step in range(1, 16):
        other, where = xy_peer(step)
        copy = remote(mine.at[other], box.at[step], xs.at[step], xr.at[step], **where)
        copy.start()
        spread.append(copy)

    for copy in corners:
        copy.wait()
    for side, strip in ((0, pl.ds(0, HALF)), (1, pl.ds(HALF + TC, HALF))):
        hout[side, :, pl.ds(0, HALF)] = canvas[:, pl.ds(HALF, HALF), strip] + cin[2 * side + 1]
        hout[side, :, pl.ds(HALF, HALF)] = canvas[:, pl.ds(TR, HALF), strip] + cin[2 * side]
    across = [
        remote(hout.at[0], hin.at[0], hs.at[0], hr.at[0], tx=left),
        remote(hout.at[1], hin.at[1], hs.at[1], hr.at[1], tx=right),
    ]
    for copy in across:
        copy.start()

    for copy in spread:
        copy.wait()
    total = mine[me]
    for step in range(1, 16):
        total = total + box[step]
    part[...] = total

    goal = me // 2
    @pl.when(z != goal)
    def _():
        at = lax.rem(goal - z + 8, 8)
        copy = remote(part, zbox.at[at], zs.at[0], zr.at[at], ty=2 * goal + core)
        copy.start()
        copy.wait_send()

    @pl.when(z == goal)
    def _():
        total = part[...]
        for step in range(1, 8):
            remote(part, zbox.at[step], zs.at[0], zr.at[step], ty=ty).wait_recv()
        for step in range(1, 8):
            total = total + zbox[step]
        final[...] = total
        keep = pltpu.make_async_copy(final, whole.at[lax.rem(me, 2)], zs.at[1])
        keep.start()
        copies = []
        for step in range(1, 16):
            other, where = xy_peer(step)
            copy = remote(final, whole.at[lax.rem(me, 2)], bs.at[step], br.at[lax.rem(me, 2)], **where)
            copy.start()
            copies.append(copy)
        keep.wait()
        for copy in copies:
            copy.wait_send()

    for half in range(2):
        @pl.when(me != 2 * z + half)
        def _():
            remote(final, whole.at[half], bs.at[0], br.at[half], tx=left).wait_recv()

    for half in range(2):
        for channel in range(3):
            psum[channel, pl.ds(8 * half, 8)] = whole[half, channel]

    for copy in sent:
        copy.wait()
    top = peak_in[...]
    for step in range(1, 16):
        top = jnp.maximum(top, pkxy[step])
    pk[0] = top
    pk[1] = jnp.broadcast_to(jnp.max(whole[:, 2]), (8, HALF))
    sent = []
    for step in range(1, 16):
        other, where = ty_peer(step)
        copy = remote(pk, pkty.at[step], ts.at[step], tr.at[step], **where)
        copy.start()
        sent.append(copy)

    for copy in ends:
        copy.wait()
    folded[:, pl.ds(0, HALF)] = canvas[:, pl.ds(HALF, HALF), cols] + vin[1]
    folded[:, pl.ds(HALF, HALF)] = canvas[:, pl.ds(TR, HALF), cols] + vin[0]
    for copy in across:
        copy.wait()
    folded[:, :, pl.ds(TC - HALF, HALF)] += hin[0]
    folded[:, :, pl.ds(0, HALF)] += hin[1]
    for copy in sent:
        copy.wait()
    top = pk[...]
    for step in range(1, 16):
        top = jnp.maximum(top, pkty[step])
    peaks[...] = top


def vmem():
    return pl.BlockSpec(memory_space=pltpu.VMEM)


def dma(*shape):
    return pltpu.SemaphoreType.DMA(shape)


def body(object_slices, probe_field, positions, live_slots, photon_counts):
    tile = object_slices[0]
    line = jnp.concatenate([positions.reshape(-1), live_slots.reshape(-1)])
    meta = jnp.pad(line, (0, HALF - 9)).reshape(1, HALF)
    wide, around = pl.pallas_call(
        halo_kernel,
        name="halo",
        out_shape=(
            jax.ShapeDtypeStruct((2, WR, WC), F32),
            jax.ShapeDtypeStruct((3, 3, 1, HALF), jnp.int32),
        ),
        in_specs=[pl.BlockSpec(memory_space=pl.ANY), vmem()],
        out_specs=(vmem(), vmem()),
        scratch_shapes=[dma(2), dma(2), dma(2), dma(2), dma(4), dma(4), dma(4), dma(4), dma(2)],
        compiler_params=pltpu.CompilerParams(
            collective_id=0, has_side_effects=True, vmem_limit_bytes=8 << 20
        ),
    )(tile, meta)
    canvas, sums, den, peak = pl.pallas_call(
        patch_kernel,
        name="patch",
        out_shape=(
            jax.ShapeDtypeStruct((2, WR, WC), F32),
            jax.ShapeDtypeStruct((2, 16, 3, 8, SIZE), F32),
            jax.ShapeDtypeStruct((TR, TC), F32),
            jax.ShapeDtypeStruct((8, HALF), F32),
        ),
        in_specs=[pl.BlockSpec(memory_space=pltpu.SMEM)] + [vmem()] * 6,
        out_specs=(vmem(),) * 4,
        scratch_shapes=[pltpu.VMEM((3 * SIZE, 13 * HALF), F32), pltpu.VMEM((SIZE, SIZE), F32)],
        compiler_params=pltpu.CompilerParams(vmem_limit_bytes=40 << 20),
    )(
        around, wide, probe_field, photon_counts[0, 0, 0],
        jnp.asarray(TABLE_HIGH), jnp.asarray(TABLE_LOW), jnp.asarray(TABLE_ORDER),
    )
    piece = (3, 8, SIZE)
    small = (8, HALF)
    folded, psum, peaks = pl.pallas_call(
        return_kernel,
        name="back",
        out_shape=(
            jax.ShapeDtypeStruct((2, TR, TC), F32),
            jax.ShapeDtypeStruct((3, 16, SIZE), F32),
            jax.ShapeDtypeStruct((2,) + small, F32),
        ),
        in_specs=[vmem()] * 3,
        out_specs=(vmem(),) * 3,
        scratch_shapes=[
            pltpu.VMEM((16,) + piece, F32),
            pltpu.VMEM((16,) + piece, F32),
            pltpu.VMEM((16,) + piece, F32),
            pltpu.VMEM(piece, F32),
            pltpu.VMEM((8,) + piece, F32),
            pltpu.VMEM((2,) + piece, F32),
            pltpu.VMEM(piece, F32),
            pltpu.VMEM((2,) + small, F32),
            pltpu.VMEM((16,) + small, F32),
            pltpu.VMEM((16, 2) + small, F32),
            pltpu.VMEM((2, 2, HALF, TC), F32),
            pltpu.VMEM((4, 2, HALF, HALF), F32),
            pltpu.VMEM((2, 2, TR, HALF), F32),
            pltpu.VMEM((2, 2, TR, HALF), F32),
            dma(2), dma(2), dma(4), dma(4), dma(2), dma(2), dma(1), dma(1),
            dma(16), dma(16), dma(2), dma(8), dma(16), dma(2), dma(16), dma(16), dma(16), dma(16),
        ],
        compiler_params=pltpu.CompilerParams(
            collective_id=1, has_side_effects=True, vmem_limit_bytes=24 << 20
        ),
    )(canvas, sums, peak)
    scale = 1.0 / (den + 0.1 * peaks[0, 0, 0])
    new_tile = tile + folded * scale[None]
    rows_each = SIZE // N_TY
    start = lax.axis_index("ty") * rows_each
    own = lax.dynamic_slice_in_dim(probe_field, start, rows_each, 1)
    new_probe = own + psum[:2] * (1.0 / (psum[2] + 0.1 * peaks[1, 0, 0]))[None]
    return (new_tile[None], new_probe)


def solution(mesh):
    placed = (
        P("angle", None, "ty", "tx"),
        P(),
        P("angle", "ty", "tx", None, None),
        P("angle", "ty", "tx"),
        P("angle", "ty", "tx", None, None, None),
    )
    return jax.shard_map(
        body,
        mesh=mesh,
        in_specs=placed,
        out_specs=(P("angle", None, "ty", "tx"), P(None, "ty", None)),
        check_vma=False,
    )
```

```python
import functools
import math

import jax
import jax.numpy as jnp
import numpy as np
from jax import lax
from jax.experimental import pallas as pl
from jax.experimental.pallas import tpu as pltpu
from jax.sharding import PartitionSpec as P

MESH = pl.DeviceIdType.MESH
F32 = jnp.float32
BF16 = jnp.bfloat16
SIZE = 256
HALF = 128
TR = 256
TC = 1024
WR = TR + SIZE
WC = TC + SIZE
N_TY = 16
N_TX = 8
N_ANGLE = 2
N_XY = N_ANGLE * N_TX


def tables():
    n = np.arange(HALF)
    base = np.exp(-2j * np.pi * np.outer(n, n) / HALF) / 16.0
    odd = base * np.exp(-2j * np.pi * n / SIZE)[None, :]

    def real_form(m):
        return np.block([[m.real, -m.imag], [m.imag, m.real]])

    mats = [real_form(base), real_form(odd)]
    mats = np.stack([mats[0], mats[1], mats[0].T, mats[1].T]).astype(np.float32)
    high = mats.astype(jnp.bfloat16)
    low = (mats - high.astype(np.float32)).astype(jnp.bfloat16)
    order = np.zeros((SIZE, SIZE), np.float32)
    for j in range(SIZE):
        order[2 * j if j < HALF else 2 * (j - HALF) + 1, j] = 1.0
    both = np.stack([order, order.T]).astype(jnp.bfloat16)
    return high, low, both


TABLE_HIGH, TABLE_LOW, TABLE_ORDER = tables()


def remote(src, dst, send, recv, **where):
    return pltpu.make_async_remote_copy(
        src_ref=src, dst_ref=dst, send_sem=send, recv_sem=recv, device_id=where, device_id_type=MESH
    )


def split(x):
    high = x.astype(BF16)
    return high, (x - high.astype(F32)).astype(BF16)


def dot(a, b):
    return jnp.dot(a, b, preferred_element_type=F32)


class Copies:
    def __init__(self, send, recv):
        self.send, self.recv, self.at = send, recv, 0

    def make(self, src, dst, **where):
        copy = remote(src, dst, self.send.at[self.at], self.recv.at[self.at], **where)
        self.at += 1
        return copy


def step_kernel(
    tile, meta, probe_h, counts_h, high_h, low_h, order_h, new_tile, new_probe,
    wide, probe, counts, high, low, order, around, around_s, padded, den, patches,
    canvas, vin, cin, hin, hout, pk_own, pk_xy, pk, pk_ty,
    den_sums, den_pair, den_mine, den_box, den_part, den_zbox, den_final, den_whole,
    num_sums, num_pair, num_mine, num_box, num_part, num_zbox, num_final, num_whole,
    send, recv, local,
):
    angle, ty, tx = lax.axis_index("angle"), lax.axis_index("ty"), lax.axis_index("tx")
    up, down = lax.rem(ty + N_TY - 1, N_TY), lax.rem(ty + 1, N_TY)
    left, right = lax.rem(tx + N_TX - 1, N_TX), lax.rem(tx + 1, N_TX)
    me = angle * N_TX + tx
    core, z = lax.rem(ty, 2), ty // 2
    goal, half = me // 2, lax.rem(me, 2)
    copies = Copies(send, recv)

    def xy_peer(step):
        other = lax.rem(me + step, N_XY)
        return other, {"angle": other // N_TX, "tx": lax.rem(other, N_TX)}

    def ty_peer(step):
        return {"ty": lax.rem(ty + step, N_TY)}

    barrier = pltpu.get_barrier_semaphore()
    for step in range(1, 16):
        pl.semaphore_signal(barrier, inc=1, device_id=xy_peer(step)[1], device_id_type=MESH)
        pl.semaphore_signal(barrier, inc=1, device_id=ty_peer(step), device_id_type=MESH)

    middle_blocks, middle_groups = pl.ds(1, 8), pl.ds(16, 32)
    top_in, bottom_in = pl.ds(16, 16), pl.ds(32, 16)
    top_out, bottom_out = pl.ds(0, 16), pl.ds(48, 16)
    middle = [
        pltpu.make_async_copy(
            tile.at[:, :, :, pl.ds(block * HALF, HALF)], wide.at[1 + block, :, middle_groups], local.at[10 + block]
        )
        for block in range(8)
    ]
    own = pltpu.make_async_copy(meta, around.at[1, 1], local.at[1])
    loads = [
        pltpu.make_async_copy(src, dst, local.at[2 + k])
        for k, (src, dst) in enumerate(
            ((probe_h, probe), (high_h, high), (low_h, low), (order_h, order), (counts_h, counts))
        )
    ]
    for copy in middle:
        copy.start()
    own.start()
    for load in loads:
        load.start()

    def clear(item, carry):
        padded[item // 16, lax.rem(item // 4, 4), lax.rem(item, 4)] = jnp.zeros((96, 8, HALF), F32)
        return carry

    lax.fori_loop(0, 32, clear, 0)
    own.wait()
    for copy in middle:
        copy.wait()
    pl.semaphore_wait(barrier, 30)

    meta_sides = [
        copies.make(meta, around.at[1, 2], tx=left),
        copies.make(meta, around.at[1, 0], tx=right),
    ]
    sides = [
        copies.make(wide.at[1, :, middle_groups], wide.at[9, :, middle_groups], tx=left),
        copies.make(wide.at[8, :, middle_groups], wide.at[0, :, middle_groups], tx=right),
    ]
    ends = [
        copies.make(wide.at[middle_blocks, :, top_in], wide.at[middle_blocks, :, bottom_out], ty=up),
        copies.make(wide.at[middle_blocks, :, bottom_in], wide.at[middle_blocks, :, top_out], ty=down),
    ]
    for copy in meta_sides + sides + ends:
        copy.start()
    for copy in meta_sides:
        copy.wait()
    meta_ends = [
        copies.make(around.at[1], around.at[2], ty=up),
        copies.make(around.at[1], around.at[0], ty=down),
    ]
    for copy in meta_ends:
        copy.start()
    for copy in meta_ends:
        copy.wait()
    scalars = pltpu.make_async_copy(around, around_s, local.at[7])
    scalars.start()
    scalars.wait()

    lane33 = lax.broadcasted_iota(jnp.int32, (33, 8, HALF), 2)
    lane32 = lax.broadcasted_iota(jnp.int32, (32, 8, HALF), 2)
    sub33 = lax.broadcasted_iota(jnp.int32, (33, 8, HALF), 1)
    sub32 = lax.broadcasted_iota(jnp.int32, (32, 8, HALF), 1)
    blank = jnp.zeros((1, 8, HALF), F32)

    def lay(channel, slot, by_row, by_col, x):
        def turned(part):
            return pltpu.roll(pltpu.roll(part.reshape(32, 8, HALF), by_col, 2), by_row, 1)

        one, two = turned(x[:, :HALF]), turned(x[:, HALF:])
        inside = lane32 >= by_col
        below = sub33 >= by_row
        zero = jnp.zeros_like(one)
        for step, part in enumerate(
            (jnp.where(inside, one, zero), jnp.where(inside, two, one), jnp.where(inside, zero, two))
        ):
            moved = jnp.where(
                below, jnp.concatenate([part, blank], 0), jnp.concatenate([blank, part], 0)
            )
            padded[channel, slot, 1 + step, pl.ds(32, 33)] = moved

    def fetch(channel, spots, block, first, count, put):
        where = []
        for slot in range(4):
            at_group, at_block = spots[slot]
            near = block - at_block
            where.append((jnp.where((near >= 0) & (near <= 2), near + 1, 0), 32 + first - at_group))
        for step in range(count):
            total = None
            for slot, (index, start) in enumerate(where):
                part = padded[channel, slot, index, start + step]
                total = part if total is None else total + part
            put(step, total)

    def group(dy, dx, begin):
        spots = []
        for slot in range(4):
            row = around_s[dy + 1, dx + 1, 0, 2 * slot] - ty * TR
            col = around_s[dy + 1, dx + 1, 0, 2 * slot + 1] - tx * TC
            used = slot < around_s[dy + 1, dx + 1, 0, 8]
            near = (row > -SIZE) & (row < TR) & (col > -SIZE) & (col < TC)
            weight = jnp.where(used & near, 1.0, 0.0).astype(F32)
            row = jnp.clip(row, -SIZE, TR - 1) + SIZE
            col = jnp.clip(col, -SIZE, TC - 1) + SIZE
            at_group, by_row = row // 8, lax.rem(row, 8)
            at_block, by_col = col // HALF, lax.rem(col, HALF)
            qr, qi = probe[0], probe[1]
            lay(0, slot, by_row, by_col, (qr * qr + qi * qi) * weight)
            spots.append((at_group - 32, at_block - 2))
        first, count = {-1: (0, 16), 0: (0, 32), 1: (16, 16)}[dy]
        begin_block, end_block = {-1: (0, 1), 0: (0, 8), 1: (7, 8)}[dx]

        def one_block(block, carry):
            def put(step, total):
                if begin:
                    den[block, first + step] = total
                else:
                    den[block, first + step] += total

            fetch(0, spots, block, first, count, put)
            return carry

        lax.fori_loop(begin_block, end_block, one_block, 0)

    loads[0].wait()
    group(0, 0, True)
    for dy, dx in ((-1, 0), (1, 0), (0, -1), (0, 1)):
        group(dy, dx, False)
    corners = []
    for side, block in ((0, 0), (1, 9)):
        sides[1 - side].wait_recv()
        for src, dst, where in ((top_in, bottom_out, {"ty": up}), (bottom_in, top_out, {"ty": down})):
            corners.append(copies.make(wide.at[block, :, src], wide.at[block, :, dst], **where))
            corners[-1].start()
    for dy, dx in ((-1, -1), (-1, 1), (1, -1), (1, 1)):
        group(dy, dx, False)
    pk_own[...] = jnp.broadcast_to(jnp.max(den[...]), (8, HALF))
    pk_copies = []
    for step in range(1, 16):
        pk_copies.append(copies.make(pk_own, pk_xy.at[step], **xy_peer(step)[1]))
        pk_copies[-1].start()
    for side in sides:
        side.wait_send()
    for copy in ends + corners:
        copy.wait()

    den_sums[...] = jnp.zeros_like(den_sums)
    num_sums[...] = jnp.zeros_like(num_sums)

    def place_of(slot):
        row = jnp.clip(around_s[1, 1, 0, 2 * slot] - (ty * TR - HALF), 0, TR - 1)
        col = jnp.clip(around_s[1, 1, 0, 2 * slot + 1] - (tx * TC - HALF), 0, TC - 1)
        return row // 8, lax.rem(row, 8), col // HALF, lax.rem(col, HALF)

    def weight_of(slot):
        return jnp.where(slot < around_s[1, 1, 0, 8], 1.0, 0.0).astype(F32)

    def add_rows(sums, channel, x):
        x = x.reshape(8, 2, 2, 8, SIZE)
        for parity in range(2):
            sums[parity, :, channel] += x[:, parity].reshape(16, 8, SIZE)

    def cut(slot, carry):
        at_group, by_row, at_block, by_col = place_of(slot)
        back_row, back_col = lax.rem(8 - by_row, 8), lax.rem(HALF - by_col, HALF)
        power = None
        for channel in range(2):
            parts = []
            for step in range(3):
                x = jnp.stack([wide[at_block + step, channel, at_group + k] for k in range(33)])
                parts.append(pltpu.roll(x, back_col, 2))
            done = []
            for step in range(2):
                x = jnp.where(lane33 < HALF - by_col, parts[step], parts[step + 1])
                x = pltpu.roll(x, back_row, 1)
                x = jnp.where(sub32 < 8 - by_row, x[:32], x[1:])
                done.append(x.reshape(SIZE, HALF))
            x = jnp.concatenate(done, 1)
            patches[slot, channel] = x
            power = x * x if power is None else power + x * x
        add_rows(den_sums, 0, power * weight_of(slot))
        return carry

    lax.fori_loop(0, 4, cut, 0)

    class Chain:
        def __init__(self, sums, pair, mine, box, part, zbox, final, whole, sem):
            self.__dict__.update(
                sums=sums, pair=pair, mine=mine, box=box, part=part, zbox=zbox, final=final, whole=whole
            )
            self.keep = pltpu.make_async_copy(final, whole.at[half], local.at[sem])
            self.over_pair = copies.make(sums.at[1 - core], pair, ty=ty + 1 - 2 * core)
            self.over_xy = [
                copies.make(mine.at[xy_peer(step)[0]], box.at[step], **xy_peer(step)[1]) for step in range(1, 16)
            ]
            base = copies.at
            far = lax.rem(goal - z + 8, 8)
            self.to_goal = remote(part, zbox.at[far], send.at[base], recv.at[base + far], ty=2 * goal + core)
            self.at_goal = [
                remote(part, zbox.at[step], send.at[base], recv.at[base + step], ty=up) for step in range(1, 8)
            ]
            base += 8
            self.out = [
                remote(final, whole.at[half], send.at[base + step], recv.at[base + half], **xy_peer(step)[1])
                for step in range(1, 16)
            ]
            self.into = [
                remote(final, whole.at[k], send.at[base], recv.at[base + k], tx=left) for k in range(2)
            ]
            copies.at = base + 16

        def start_pair(self):
            self.over_pair.start()

        def start_xy(self):
            self.over_pair.wait()
            self.mine[...] = self.sums[core] + self.pair[...]
            for copy in self.over_xy:
                copy.start()

        def start_z(self):
            for copy in self.over_xy:
                copy.wait()
            total = self.mine[me]
            for step in range(1, 16):
                total = total + self.box[step]
            self.part[...] = total

            @pl.when(z != goal)
            def _():
                self.to_goal.start()

        def start_out(self):
            @pl.when(z != goal)
            def _():
                self.to_goal.wait_send()

            @pl.when(z == goal)
            def _():
                for copy in self.at_goal:
                    copy.wait_recv()
                total = self.part[...]
                for step in range(1, 8):
                    total = total + self.zbox[step]
                self.final[...] = total
                self.keep.start()
                for copy in self.out:
                    copy.start()

        def finish(self):
            @pl.when(z == goal)
            def _():
                self.keep.wait()
                for copy in self.out:
                    copy.wait_send()

            for k in range(2):
                @pl.when(me != 2 * z + k)
                def _():
                    self.into[k].wait_recv()

    den_chain = Chain(den_sums, den_pair, den_mine, den_box, den_part, den_zbox, den_final, den_whole, 8)
    num_chain = Chain(num_sums, num_pair, num_mine, num_box, num_part, num_zbox, num_final, num_whole, 9)
    den_chain.start_pair()
    for load in loads[1:]:
        load.wait()

    def from_left(which, x):
        a, b = split(x)
        return dot(high[which], a) + (dot(high[which], b) + dot(low[which], a))

    def from_right(x, which):
        a, b = split(x)
        return dot(a, high[which]) + (dot(b, high[which]) + dot(a, low[which]))

    def one_slot(slot, carry):
        at_group, by_row, at_block, by_col = place_of(slot)
        weight = weight_of(slot)
        xr, xi = patches[slot, 0], patches[slot, 1]
        qr, qi = probe[0], probe[1]
        pr, pi = qr * xr - qi * xi, qr * xi + qi * xr
        even = from_right(
            jnp.concatenate([pr[:, :HALF] + pr[:, HALF:], pi[:, :HALF] + pi[:, HALF:]], 1), 2
        )
        odd = from_right(
            jnp.concatenate([pr[:, :HALF] - pr[:, HALF:], pi[:, :HALF] - pi[:, HALF:]], 1), 3
        )
        mr = jnp.concatenate([even[:, :HALF], odd[:, :HALF]], 1)
        mi = jnp.concatenate([even[:, HALF:], odd[:, HALF:]], 1)
        fe = from_left(0, jnp.concatenate([mr[:HALF] + mr[HALF:], mi[:HALF] + mi[HALF:]], 0))
        fo = from_left(1, jnp.concatenate([mr[:HALF] - mr[HALF:], mi[:HALF] - mi[HALF:]], 0))
        count = counts[slot]
        tens = lax.shift_right_logical(count, 4)
        ones = count - 16 * tens
        tens = dot(dot(order[1], tens.astype(F32).astype(BF16)).astype(BF16), order[0])
        ones = dot(dot(order[1], ones.astype(F32).astype(BF16)).astype(BF16), order[0])
        count = 16.0 * tens + ones

        def scaled(f, c):
            re, im = f[:HALF], f[HALF:]
            size = jnp.maximum(re * re + im * im, 0.0625)
            factor = (0.05 * c) * lax.rsqrt(c * size)
            return jnp.concatenate([re * factor, im * factor], 0)

        ge = from_left(2, scaled(fe, count[:HALF]))
        go = from_left(3, scaled(fo, count[HALF:]))
        top, bottom = ge + go, ge - go
        hr_ = jnp.concatenate([top[:HALF], bottom[:HALF]], 0)
        hi_ = jnp.concatenate([top[HALF:], bottom[HALF:]], 0)
        be = from_right(jnp.concatenate([hr_[:, :HALF], hi_[:, :HALF]], 1), 0)
        bo = from_right(jnp.concatenate([hr_[:, HALF:], hi_[:, HALF:]], 1), 1)
        first, second = be + bo, be - bo
        dr = (jnp.concatenate([first[:, :HALF], second[:, :HALF]], 1) - pr) * weight
        di = (jnp.concatenate([first[:, HALF:], second[:, HALF:]], 1) - pi) * weight
        lay(0, slot, by_row, by_col, qr * dr + qi * di)
        lay(1, slot, by_row, by_col, qr * di - qi * dr)
        add_rows(num_sums, 0, xr * dr + xi * di)
        add_rows(num_sums, 1, xr * di - xi * dr)
        return carry

    lax.fori_loop(0, 1, one_slot, 0)
    den_chain.start_xy()
    lax.fori_loop(1, 4, one_slot, 0)
    num_chain.start_pair()

    places = [(place_of(slot)[0], place_of(slot)[2]) for slot in range(4)]

    def one_canvas(block, carry):
        for channel in range(2):
            def put(step, total):
                canvas[block, channel, step] = total

            fetch(channel, places, block, 0, 64, put)
        return carry

    lax.fori_loop(0, 2, lambda k, carry: one_canvas(9 * k, carry), 0)
    back_corners = []
    for side, block in ((0, 0), (1, 9)):
        for way, (src, where) in enumerate(((top_out, {"ty": up}), (bottom_out, {"ty": down}))):
            back_corners.append(copies.make(canvas.at[block, :, src], cin.at[2 * side + way], **where))
            back_corners[-1].start()
    lax.fori_loop(1, 9, one_canvas, 0)
    back_ends = [
        [
            copies.make(canvas.at[middle_blocks, channel, top_out], vin.at[0, channel], ty=up),
            copies.make(canvas.at[middle_blocks, channel, bottom_out], vin.at[1, channel], ty=down),
        ]
        for channel in range(2)
    ]
    for copy in back_ends[0]:
        copy.start()
    den_chain.start_z()
    num_chain.start_xy()
    for copy in back_corners:
        copy.wait()
    for side, block in ((0, 0), (1, 9)):
        hout[side, :, pl.ds(0, 16)] = canvas[block, :, top_in] + cin[2 * side + 1]
        hout[side, :, pl.ds(16, 16)] = canvas[block, :, bottom_in] + cin[2 * side]
    across = [
        copies.make(hout.at[0], hin.at[0], tx=left),
        copies.make(hout.at[1], hin.at[1], tx=right),
    ]
    for copy in across:
        copy.start()
    den_chain.start_out()
    num_chain.start_z()
    for copy in back_ends[1]:
        copy.start()
    for copy in pk_copies:
        copy.wait()
    top = pk_own[...]
    for step in range(1, 16):
        top = jnp.maximum(top, pk_xy[step])
    pk[0] = top
    den_chain.finish()
    pk[1] = jnp.broadcast_to(jnp.max(den_whole[...]), (8, HALF))
    pk_copies = []
    for step in range(1, 16):
        pk_copies.append(copies.make(pk, pk_ty.at[step], **ty_peer(step)))
        pk_copies[-1].start()
    num_chain.start_out()
    for copy in pk_copies:
        copy.wait()
    top = pk[...]
    for step in range(1, 16):
        top = jnp.maximum(top, pk_ty[step])
    peak_obj, peak_probe = top[0, 0, 0], top[1, 0, 0]
    den[...] = 1.0 / (den[...] + 0.1 * peak_obj)
    for copy in across:
        copy.wait()
    for block, side in ((8, 0), (1, 1)):
        canvas[block, :, middle_groups] += hin[side]
    for channel in range(2):
        for copy in back_ends[channel]:
            copy.wait()
        for first, side in ((0, 1), (16, 0)):
            here, there = pl.ds(16 + first, 16), pl.ds(first, 16)
            for block in range(8):
                value = canvas[1 + block, channel, here] + vin[side, channel, block]
                new_tile[channel, there, :, pl.ds(block * HALF, HALF)] = (
                    wide[1 + block, channel, here] + value * den[block, there]
                )
    num_chain.finish()
    for k in range(2):
        rows = pl.ds(pl.multiple_of(16 * ty + 8 * k, 8), 8)
        scale = 1.0 / (den_whole[k, 0] + 0.1 * peak_probe)
        for channel in range(2):
            new_probe[channel, pl.ds(8 * k, 8)] = probe[channel, rows, :] + num_whole[k, channel] * scale


def vmem():
    return pl.BlockSpec(memory_space=pltpu.VMEM)


def chain_scratch(channels):
    piece = (channels, 8, SIZE)
    shapes = ((2, 16) + piece, (16,) + piece, (16,) + piece, (16,) + piece, piece, (8,) + piece, piece, (2,) + piece)
    return [pltpu.VMEM(shape, F32) for shape in shapes]


def body(object_slices, probe_field, positions, live_slots, photon_counts):
    line = jnp.concatenate([positions.reshape(-1), live_slots.reshape(-1)])
    meta = jnp.pad(line, (0, HALF - 9)).reshape(1, HALF)
    small = (8, HALF)
    new_tile, new_probe = pl.pallas_call(
        step_kernel,
        name="step",
        out_shape=(
            jax.ShapeDtypeStruct((2, 32, 8, TC), F32),
            jax.ShapeDtypeStruct((2, 16, SIZE), F32),
        ),
        in_specs=[pl.BlockSpec(memory_space=pltpu.HBM), vmem()] + [pl.BlockSpec(memory_space=pltpu.HBM)] * 5,
        out_specs=(vmem(), vmem()),
        scratch_shapes=[
            pltpu.VMEM((10, 2, 64, 8, HALF), F32),
            pltpu.VMEM((2, SIZE, SIZE), F32),
            pltpu.VMEM((4, SIZE, SIZE), jnp.int32),
            pltpu.VMEM((4, SIZE, SIZE), BF16),
            pltpu.VMEM((4, SIZE, SIZE), BF16),
            pltpu.VMEM((2, SIZE, SIZE), BF16),
            pltpu.VMEM((3, 3, 1, HALF), jnp.int32),
            pltpu.SMEM((3, 3, 1, HALF), jnp.int32),
            pltpu.VMEM((2, 4, 4, 96, 8, HALF), F32),
            pltpu.VMEM((8, 32, 8, HALF), F32),
            pltpu.VMEM((4, 2, SIZE, SIZE), F32),
            pltpu.VMEM((10, 2, 64, 8, HALF), F32),
            pltpu.VMEM((2, 2, 8, 16, 8, HALF), F32),
            pltpu.VMEM((4, 2, 16, 8, HALF), F32),
            pltpu.VMEM((2, 2, 32, 8, HALF), F32),
            pltpu.VMEM((2, 2, 32, 8, HALF), F32),
            pltpu.VMEM(small, F32),
            pltpu.VMEM((16,) + small, F32),
            pltpu.VMEM((2,) + small, F32),
            pltpu.VMEM((16, 2) + small, F32),
            *chain_scratch(1),
            *chain_scratch(2),
            pltpu.SemaphoreType.DMA((144,)),
            pltpu.SemaphoreType.DMA((144,)),
            pltpu.SemaphoreType.DMA((18,)),
        ],
        compiler_params=pltpu.CompilerParams(
            collective_id=0, has_side_effects=True, vmem_limit_bytes=46 << 20
        ),
    )(
        object_slices.reshape(2, 32, 8, TC), meta, probe_field, photon_counts[0, 0, 0],
        jnp.asarray(TABLE_HIGH), jnp.asarray(TABLE_LOW), jnp.asarray(TABLE_ORDER),
    )
    return (new_tile.reshape(1, 2, TR, TC), new_probe)


def solution(mesh):
    placed = (
        P("angle", None, "ty", "tx"),
        P(),
        P("angle", "ty", "tx", None, None),
        P("angle", "ty", "tx"),
        P("angle", "ty", "tx", None, None, None),
    )
    return jax.shard_map(
        body,
        mesh=mesh,
        in_specs=placed,
        out_specs=(P("angle", None, "ty", "tx"), P(None, "ty", None)),
        check_vma=False,
    )
```

```python
import functools
import math

import jax
import jax.numpy as jnp
import numpy as np
from jax import lax
from jax.experimental import pallas as pl
from jax.experimental.pallas import tpu as pltpu
from jax.sharding import PartitionSpec as P

MESH = pl.DeviceIdType.MESH
F32 = jnp.float32
BF16 = jnp.bfloat16
SIZE = 256
HALF = 128
TR = 256
TC = 1024
WR = TR + SIZE
WC = TC + SIZE
N_TY = 16
N_TX = 8
N_ANGLE = 2
N_XY = N_ANGLE * N_TX


def tables():
    n = np.arange(HALF)
    base = np.exp(-2j * np.pi * np.outer(n, n) / HALF) / 16.0
    odd = base * np.exp(-2j * np.pi * n / SIZE)[None, :]

    def real_form(m):
        return np.block([[m.real, -m.imag], [m.imag, m.real]])

    mats = [real_form(base), real_form(odd)]
    mats = np.stack([mats[0], mats[1], mats[0].T, mats[1].T]).astype(np.float32)
    high = mats.astype(jnp.bfloat16)
    low = (mats - high.astype(np.float32)).astype(jnp.bfloat16)
    order = np.zeros((SIZE, SIZE), np.float32)
    for j in range(SIZE):
        order[2 * j if j < HALF else 2 * (j - HALF) + 1, j] = 1.0
    both = np.stack([order, order.T]).astype(jnp.bfloat16)
    return high, low, both


TABLE_HIGH, TABLE_LOW, TABLE_ORDER = tables()


def remote(src, dst, send, recv, **where):
    return pltpu.make_async_remote_copy(
        src_ref=src, dst_ref=dst, send_sem=send, recv_sem=recv, device_id=where, device_id_type=MESH
    )


def split(x):
    high = x.astype(BF16)
    return high, (x - high.astype(F32)).astype(BF16)


def dot(a, b):
    return jnp.dot(a, b, preferred_element_type=F32)


class Copies:
    def __init__(self, send, recv):
        self.send, self.recv, self.at = send, recv, 0

    def make(self, src, dst, **where):
        copy = remote(src, dst, self.send.at[self.at], self.recv.at[self.at], **where)
        self.at += 1
        return copy


def step_kernel(
    spots_s, live_s, tile, probe_h, counts_h, high_h, low_h, order_h, new_tile, new_probe,
    wide, probe, counts, high, low, order, around, around_s, power, padded, den, patches,
    canvas, vin, cin, hin, hout, pk_x, pk_x_in, pk_y, pk_y_in, pk, pk_z_in, pk_pair, pk_pair_in,
    den_sums, den_pair, den_mine, den_box, den_part, den_zbox, den_ybox, den_whole,
    num_sums, num_pair, num_mine, num_box, num_part, num_zbox, num_ybox, num_whole,
    send, recv, local,
):
    angle, ty, tx = lax.axis_index("angle"), lax.axis_index("ty"), lax.axis_index("tx")
    up, down = lax.rem(ty + N_TY - 1, N_TY), lax.rem(ty + 1, N_TY)
    left, right = lax.rem(tx + N_TX - 1, N_TX), lax.rem(tx + 1, N_TX)
    core, z = lax.rem(ty, 2), ty // 2
    x, y = tx // 2, 2 * angle + lax.rem(tx, 2)
    copies = Copies(send, recv)
    pair = {"ty": ty + 1 - 2 * core}

    def x_peer(step):
        other = lax.rem(x + step, 4)
        return other, {"tx": 2 * other + lax.rem(tx, 2)}

    def y_peer(step):
        other = lax.rem(y + step, 4)
        return other, {"angle": other // 2, "tx": 2 * x + lax.rem(other, 2)}

    def z_peer(step):
        other = lax.rem(z + step, 8)
        return other, {"ty": 2 * other + core}

    greeted = [{"tx": left}, {"tx": right}, {"ty": up}, {"ty": down}, pair]
    greeted += [x_peer(step)[1] for step in (1, 2, 3)] + [y_peer(step)[1] for step in (1, 2, 3)]
    greeted += [z_peer(step)[1] for step in range(1, 8)]
    barrier = pltpu.get_barrier_semaphore()
    for where in greeted:
        pl.semaphore_signal(barrier, inc=1, device_id=where, device_id_type=MESH)

    lane = lax.broadcasted_iota(jnp.int32, (1, HALF), 1)
    line = jnp.where(lane == 8, live_s[0, 0, 0], 0)
    for slot in range(4):
        for k in range(2):
            line = jnp.where(lane == 2 * slot + k, spots_s[0, 0, 0, slot, k], line)
    around[1, 1] = line

    middle_blocks, middle_groups = pl.ds(1, 8), pl.ds(16, 32)
    top_in, bottom_in = pl.ds(16, 16), pl.ds(32, 16)
    top_out, bottom_out = pl.ds(0, 16), pl.ds(48, 16)
    middle = [
        pltpu.make_async_copy(
            tile.at[:, :, :, pl.ds(block * HALF, HALF)], wide.at[1 + block, :, middle_groups], local.at[10 + block]
        )
        for block in range(8)
    ]
    loads = [
        pltpu.make_async_copy(src, dst, local.at[2 + k])
        for k, (src, dst) in enumerate(
            ((probe_h, probe), (high_h, high), (low_h, low), (order_h, order), (counts_h, counts))
        )
    ]
    for copy in middle:
        copy.start()
    for load in loads:
        load.start()

    def clear(item, carry):
        padded[item // 16, lax.rem(item // 4, 4), lax.rem(item, 4)] = jnp.zeros((96, 8, HALF), F32)
        return carry

    lax.fori_loop(0, 32, clear, 0)
    lane32 = lax.broadcasted_iota(jnp.int32, (32, 8, HALF), 2)
    lane33 = lax.broadcasted_iota(jnp.int32, (33, 8, HALF), 2)
    sub32 = lax.broadcasted_iota(jnp.int32, (32, 8, HALF), 1)
    blank = jnp.zeros((1, 8, HALF), F32)

    def lay(channel, slot, by_row, by_col, x, part_rows=0, part_cols=0):
        count = 16 if part_rows else 32
        first = 16 if part_rows == -1 else 0
        inside = lax.broadcasted_iota(jnp.int32, (count, 8, HALF), 2) >= by_col
        below = lax.broadcasted_iota(jnp.int32, (count + 1, 8, HALF), 1) >= by_row

        def turned(part):
            part = part[8 * first : 8 * (first + count)].reshape(count, 8, HALF)
            return pltpu.roll(pltpu.roll(part, by_col, 2), by_row, 1)

        zero = jnp.zeros((count, 8, HALF), F32)
        one = zero if part_cols == -1 else turned(x[:, :HALF])
        two = zero if part_cols == 1 else turned(x[:, HALF:])
        parts = (
            None if part_cols == -1 else jnp.where(inside, one, zero),
            jnp.where(inside, two, one),
            None if part_cols == 1 else jnp.where(inside, zero, two),
        )
        for step, part in enumerate(parts):
            at = padded.at[channel, slot, 1 + step]
            if part is None:
                at[pl.ds(32, 33)] = jnp.zeros((33, 8, HALF), F32)
                continue
            moved = jnp.where(
                below, jnp.concatenate([part, blank], 0), jnp.concatenate([blank, part], 0)
            )
            at[pl.ds(32 + first, count + 1)] = moved
            if part_rows == 1:
                at[pl.ds(49, 16)] = jnp.zeros((16, 8, HALF), F32)
            if part_rows == -1:
                at[pl.ds(32, 16)] = jnp.zeros((16, 8, HALF), F32)

    def fetch(channel, spots, block, first, count, put):
        where = []
        for slot in range(4):
            at_group, at_block = spots[slot]
            near = block - at_block
            where.append((jnp.where((near >= 0) & (near <= 2), near + 1, 0), 32 + first - at_group))
        for step in range(count):
            total = None
            for slot, (index, start) in enumerate(where):
                part = padded[channel, slot, index, start + step]
                total = part if total is None else total + part
            put(step, total)

    def group(dy, dx, begin):
        spots = []
        for slot in range(4):
            if begin:
                row, col, used = spots_s[0, 0, 0, slot, 0], spots_s[0, 0, 0, slot, 1], slot < live_s[0, 0, 0]
            else:
                line = around_s.at[dy + 1, dx + 1, 0]
                row, col, used = line[2 * slot], line[2 * slot + 1], slot < line[8]
            row, col = row - ty * TR, col - tx * TC
            near = (row > -SIZE) & (row < TR) & (col > -SIZE) & (col < TC)
            weight = jnp.where(used & near, 1.0, 0.0).astype(F32)
            row = jnp.clip(row, -SIZE, TR - 1) + SIZE
            col = jnp.clip(col, -SIZE, TC - 1) + SIZE
            at_group, by_row = row // 8, lax.rem(row, 8)
            at_block, by_col = col // HALF, lax.rem(col, HALF)
            lay(0, slot, by_row, by_col, power[...] * weight, dy, dx)
            spots.append((at_group - 32, at_block - 2))
        first, count = {-1: (0, 16), 0: (0, 32), 1: (16, 16)}[dy]
        begin_block, end_block = {-1: (0, 1), 0: (0, 8), 1: (7, 8)}[dx]

        def one_block(block, carry):
            def put(step, total):
                if begin:
                    den[block, first + step] = total
                else:
                    den[block, first + step] += total

            fetch(0, spots, block, first, count, put)
            return carry

        lax.fori_loop(begin_block, end_block, one_block, 0)

    loads[0].wait()
    power[...] = probe[0] * probe[0] + probe[1] * probe[1]
    for copy in middle:
        copy.wait()
    pl.semaphore_wait(barrier, len(greeted))

    meta_sides = [
        copies.make(around.at[1, 1], around.at[1, 2], tx=left),
        copies.make(around.at[1, 1], around.at[1, 0], tx=right),
    ]
    sides = [
        [
            copies.make(wide.at[1, channel, middle_groups], wide.at[9, channel, middle_groups], tx=left),
            copies.make(wide.at[8, channel, middle_groups], wide.at[0, channel, middle_groups], tx=right),
        ]
        for channel in range(2)
    ]
    ends = [
        copies.make(wide.at[middle_blocks, :, top_in], wide.at[middle_blocks, :, bottom_out], ty=up),
        copies.make(wide.at[middle_blocks, :, bottom_in], wide.at[middle_blocks, :, top_out], ty=down),
    ]
    for copy in meta_sides + sides[0] + sides[1] + ends:
        copy.start()
    for copy in meta_sides:
        copy.wait()
    meta_ends = [
        copies.make(around.at[1], around.at[2], ty=up),
        copies.make(around.at[1], around.at[0], ty=down),
    ]
    for copy in meta_ends:
        copy.start()
    group(0, 0, True)
    for copy in meta_ends:
        copy.wait()
    scalars = pltpu.make_async_copy(around, around_s, local.at[7])
    scalars.start()
    scalars.wait()

    corners = []

    def relay(channel):
        for side, block in ((0, 0), (1, 9)):
            sides[channel][1 - side].wait_recv()
            for src, dst, where in ((top_in, bottom_out, {"ty": up}), (bottom_in, top_out, {"ty": down})):
                corners.append(copies.make(wide.at[block, channel, src], wide.at[block, channel, dst], **where))
                corners[-1].start()

    for dy, dx in ((-1, 0), (1, 0)):
        group(dy, dx, False)
    relay(0)
    for dy, dx in ((0, -1), (0, 1), (-1, -1), (-1, 1)):
        group(dy, dx, False)
    relay(1)
    for dy, dx in ((1, -1), (1, 1)):
        group(dy, dx, False)
    def share(value, own, others, peers):
        own[...] = value
        sent = [copies.make(own, others.at[k], **where) for k, where in enumerate(peers)]
        for copy in sent:
            copy.start()

        def finish():
            for copy in sent:
                copy.wait()
            top = own[...]
            for k in range(len(sent)):
                top = jnp.maximum(top, others[k])
            return top

        return finish

    top_x = share(
        jnp.broadcast_to(jnp.max(den[...]), (1, HALF)), pk_x, pk_x_in, [x_peer(step)[1] for step in (1, 2, 3)]
    )
    for side in sides[0] + sides[1]:
        side.wait_send()
    for copy in ends + corners:
        copy.wait()
    top_y = share(top_x(), pk_y, pk_y_in, [y_peer(step)[1] for step in (1, 2, 3)])

    den_sums[...] = jnp.zeros_like(den_sums)
    num_sums[...] = jnp.zeros_like(num_sums)

    def place_of(slot):
        row = jnp.clip(spots_s[0, 0, 0, slot, 0] - (ty * TR - HALF), 0, TR - 1)
        col = jnp.clip(spots_s[0, 0, 0, slot, 1] - (tx * TC - HALF), 0, TC - 1)
        return row // 8, lax.rem(row, 8), col // HALF, lax.rem(col, HALF)

    def weight_of(slot):
        return jnp.where(slot < live_s[0, 0, 0], 1.0, 0.0).astype(F32)

    def add_rows(sums, channel, value):
        value = value.reshape(8, 2, 2, 8, SIZE)
        for parity in range(2):
            for quarter in range(4):
                side = HALF * (quarter % 2)
                sums[parity, quarter, :, channel] += value[:, parity, quarter // 2, :, side : side + HALF]

    def cut(slot, carry):
        at_group, by_row, at_block, by_col = place_of(slot)
        back_row, back_col = lax.rem(8 - by_row, 8), lax.rem(HALF - by_col, HALF)
        square = None
        for channel in range(2):
            parts = []
            for step in range(3):
                x = jnp.stack([wide[at_block + step, channel, at_group + k] for k in range(33)])
                parts.append(pltpu.roll(x, back_col, 2))
            done = []
            for step in range(2):
                x = jnp.where(lane33 < HALF - by_col, parts[step], parts[step + 1])
                x = pltpu.roll(x, back_row, 1)
                x = jnp.where(sub32 < 8 - by_row, x[:32], x[1:])
                done.append(x.reshape(SIZE, HALF))
            x = jnp.concatenate(done, 1)
            patches[slot, channel] = x
            square = x * x if square is None else square + x * x
        add_rows(den_sums, 0, square * weight_of(slot))
        return carry

    lax.fori_loop(0, 4, cut, 0)

    class Chain:
        def __init__(self, sums, pair_in, mine, box, part, zbox, ybox, whole):
            self.__dict__.update(sums=sums, pair_in=pair_in, mine=mine, box=box, part=part, zbox=zbox, ybox=ybox, whole=whole)
            self.over_pair = copies.make(sums.at[1 - core], pair_in, **pair)
            self.over_x = [
                copies.make(mine.at[x_peer(step)[0]], box.at[step], **x_peer(step)[1]) for step in (1, 2, 3)
            ]
            self.over_z = [
                copies.make(part.at[z_peer(step)[0]], zbox.at[step], **z_peer(step)[1]) for step in range(1, 8)
            ]
            self.over_y = [copies.make(ybox.at[y], ybox.at[y], **y_peer(step)[1]) for step in (1, 2, 3)]
            self.out = [copies.make(whole.at[x], whole.at[x], **x_peer(step)[1]) for step in (1, 2, 3)]

        def start_pair(self):
            self.over_pair.start()

        def start_x(self):
            self.over_pair.wait()
            self.mine[...] = self.sums[core] + self.pair_in[...]
            for copy in self.over_x:
                copy.start()

        def start_z(self):
            for copy in self.over_x:
                copy.wait()
            self.part[...] = self.mine[x] + self.box[1] + self.box[2] + self.box[3]
            for copy in self.over_z:
                copy.start()

        def start_y(self):
            for copy in self.over_z:
                copy.wait()
            total = self.part[z]
            for step in range(1, 8):
                total = total + self.zbox[step]
            self.ybox[y] = total
            for copy in self.over_y:
                copy.start()

        def start_out(self):
            for copy in self.over_y:
                copy.wait()
            self.whole[x] = (self.ybox[0] + self.ybox[1]) + (self.ybox[2] + self.ybox[3])
            for copy in self.out:
                copy.start()

        def finish(self):
            for copy in self.out:
                copy.wait()

    den_chain = Chain(den_sums, den_pair, den_mine, den_box, den_part, den_zbox, den_ybox, den_whole)
    num_chain = Chain(num_sums, num_pair, num_mine, num_box, num_part, num_zbox, num_ybox, num_whole)
    den_chain.start_pair()
    for load in loads[1:]:
        load.wait()

    def from_left(which, x):
        a, b = split(x)
        return dot(high[which], a) + (dot(high[which], b) + dot(low[which], a))

    def from_right(x, which):
        a, b = split(x)
        return dot(a, high[which]) + (dot(b, high[which]) + dot(a, low[which]))

    def one_slot(slot, carry):
        at_group, by_row, at_block, by_col = place_of(slot)
        weight = weight_of(slot)
        xr, xi = patches[slot, 0], patches[slot, 1]
        qr, qi = probe[0], probe[1]
        pr, pi = qr * xr - qi * xi, qr * xi + qi * xr
        even = from_right(
            jnp.concatenate([pr[:, :HALF] + pr[:, HALF:], pi[:, :HALF] + pi[:, HALF:]], 1), 2
        )
        odd = from_right(
            jnp.concatenate([pr[:, :HALF] - pr[:, HALF:], pi[:, :HALF] - pi[:, HALF:]], 1), 3
        )
        mr = jnp.concatenate([even[:, :HALF], odd[:, :HALF]], 1)
        mi = jnp.concatenate([even[:, HALF:], odd[:, HALF:]], 1)
        fe = from_left(0, jnp.concatenate([mr[:HALF] + mr[HALF:], mi[:HALF] + mi[HALF:]], 0))
        fo = from_left(1, jnp.concatenate([mr[:HALF] - mr[HALF:], mi[:HALF] - mi[HALF:]], 0))
        count = counts[slot]
        tens = lax.shift_right_logical(count, 4)
        ones = count - 16 * tens
        tens = dot(dot(order[1], tens.astype(F32).astype(BF16)).astype(BF16), order[0])
        ones = dot(dot(order[1], ones.astype(F32).astype(BF16)).astype(BF16), order[0])
        count = 16.0 * tens + ones

        def scaled(f, c):
            re, im = f[:HALF], f[HALF:]
            size = jnp.maximum(re * re + im * im, 0.0625)
            factor = (0.05 * c) * lax.rsqrt(c * size)
            return jnp.concatenate([re * factor, im * factor], 0)

        ge = from_left(2, scaled(fe, count[:HALF]))
        go = from_left(3, scaled(fo, count[HALF:]))
        top, bottom = ge + go, ge - go
        hr_ = jnp.concatenate([top[:HALF], bottom[:HALF]], 0)
        hi_ = jnp.concatenate([top[HALF:], bottom[HALF:]], 0)
        be = from_right(jnp.concatenate([hr_[:, :HALF], hi_[:, :HALF]], 1), 0)
        bo = from_right(jnp.concatenate([hr_[:, HALF:], hi_[:, HALF:]], 1), 1)
        first, second = be + bo, be - bo
        dr = (jnp.concatenate([first[:, :HALF], second[:, :HALF]], 1) - pr) * weight
        di = (jnp.concatenate([first[:, HALF:], second[:, HALF:]], 1) - pi) * weight
        lay(0, slot, by_row, by_col, qr * dr + qi * di)
        lay(1, slot, by_row, by_col, qr * di - qi * dr)
        add_rows(num_sums, 0, xr * dr + xi * di)
        add_rows(num_sums, 1, xr * di - xi * dr)
        return carry

    lax.fori_loop(0, 1, one_slot, 0)
    den_chain.start_x()
    lax.fori_loop(1, 3, one_slot, 0)
    den_chain.start_z()
    lax.fori_loop(3, 4, one_slot, 0)
    num_chain.start_pair()

    places = [(place_of(slot)[0], place_of(slot)[2]) for slot in range(4)]

    def one_canvas(first, count):
        def add(block, carry):
            for channel in range(2):
                def put(step, total):
                    canvas[block, channel, first + step] = total

                fetch(channel, places, block, first, count, put)
            return carry

        return add

    lax.fori_loop(0, 2, lambda k, carry: one_canvas(0, 64)(9 * k, carry), 0)
    back_corners = []
    for side, block in ((0, 0), (1, 9)):
        for way, (src, where) in enumerate(((top_out, {"ty": up}), (bottom_out, {"ty": down}))):
            back_corners.append(copies.make(canvas.at[block, :, src], cin.at[2 * side + way], **where))
            back_corners[-1].start()
    num_chain.start_x()
    den_chain.start_y()
    lax.fori_loop(1, 9, one_canvas(0, 16), 0)
    lax.fori_loop(1, 9, one_canvas(48, 16), 0)
    back_ends = []
    for channel in range(2):
        for part in range(2):
            blocks, there = pl.ds(1 + 4 * part, 4), pl.ds(4 * part, 4)
            back_ends.append(
                [
                    copies.make(canvas.at[blocks, channel, top_out], vin.at[0, channel, there], ty=up),
                    copies.make(canvas.at[blocks, channel, bottom_out], vin.at[1, channel, there], ty=down),
                ]
            )

    def start_ends(k):
        for copy in back_ends[k]:
            copy.start()

    start_ends(0)
    den_chain.start_out()
    for copy in back_corners:
        copy.wait()
    for side, block in ((0, 0), (1, 9)):
        hout[side, :, pl.ds(0, 16)] = canvas[block, :, top_in] + cin[2 * side + 1]
        hout[side, :, pl.ds(16, 16)] = canvas[block, :, bottom_in] + cin[2 * side]
    across = [
        copies.make(hout.at[0], hin.at[0], tx=left),
        copies.make(hout.at[1], hin.at[1], tx=right),
    ]
    for copy in across:
        copy.start()
    start_ends(1)
    num_chain.start_z()
    den_chain.finish()
    pk[0] = top_y()
    pk[1] = jnp.broadcast_to(jnp.max(den_whole[...]), (1, HALF))
    top_z = share(pk[...], pk, pk_z_in, [z_peer(step)[1] for step in range(1, 8)])
    start_ends(2)
    lax.fori_loop(1, 9, one_canvas(16, 32), 0)
    num_chain.start_y()
    start_ends(3)
    top_pair = share(top_z(), pk_pair, pk_pair_in, [pair])
    num_chain.start_out()
    top = top_pair()
    peak_obj, peak_probe = top[0, 0, 0], top[1, 0, 0]
    den[...] = 1.0 / (den[...] + 0.1 * peak_obj)
    for copy in across:
        copy.wait()
    for block, side in ((8, 0), (1, 1)):
        canvas[block, :, middle_groups] += hin[side]
    for channel in range(2):
        for copy in back_ends[2 * channel] + back_ends[2 * channel + 1]:
            copy.wait()
        for first, side in ((0, 1), (16, 0)):
            here, there = pl.ds(16 + first, 16), pl.ds(first, 16)
            for block in range(8):
                value = canvas[1 + block, channel, here] + vin[side, channel, block]
                new_tile[channel, there, :, pl.ds(block * HALF, HALF)] = (
                    wide[1 + block, channel, here] + value * den[block, there]
                )
    num_chain.finish()
    for quarter in range(4):
        rows = pl.ds(pl.multiple_of(16 * ty + 8 * (quarter // 2), 8), 8)
        cols = pl.ds(HALF * (quarter % 2), HALF)
        scale = 1.0 / (den_whole[quarter, 0] + 0.1 * peak_probe)
        for channel in range(2):
            new_probe[channel, pl.ds(8 * (quarter // 2), 8), cols] = (
                probe[channel, rows, cols] + num_whole[quarter, channel] * scale
            )


def vmem():
    return pl.BlockSpec(memory_space=pltpu.VMEM)


def chain_scratch(channels):
    piece = (channels, 8, HALF)
    shapes = (
        (2, 4, 8) + piece, (4, 8) + piece, (4, 8) + piece, (4, 8) + piece,
        (8,) + piece, (8,) + piece, (4,) + piece, (4,) + piece,
    )
    return [pltpu.VMEM(shape, F32) for shape in shapes]


def body(object_slices, probe_field, positions, live_slots, photon_counts):
    new_tile, new_probe = pl.pallas_call(
        step_kernel,
        name="step",
        out_shape=(
            jax.ShapeDtypeStruct((2, 32, 8, TC), F32),
            jax.ShapeDtypeStruct((2, 16, SIZE), F32),
        ),
        in_specs=[pl.BlockSpec(memory_space=pltpu.SMEM)] * 2 + [pl.BlockSpec(memory_space=pltpu.HBM)] * 6,
        out_specs=(vmem(), vmem()),
        scratch_shapes=[
            pltpu.VMEM((10, 2, 64, 8, HALF), F32),
            pltpu.VMEM((2, SIZE, SIZE), F32),
            pltpu.VMEM((4, SIZE, SIZE), jnp.int32),
            pltpu.VMEM((4, SIZE, SIZE), BF16),
            pltpu.VMEM((4, SIZE, SIZE), BF16),
            pltpu.VMEM((2, SIZE, SIZE), BF16),
            pltpu.VMEM((3, 3, 1, HALF), jnp.int32),
            pltpu.SMEM((3, 3, 1, HALF), jnp.int32),
            pltpu.VMEM((SIZE, SIZE), F32),
            pltpu.VMEM((2, 4, 4, 96, 8, HALF), F32),
            pltpu.VMEM((8, 32, 8, HALF), F32),
            pltpu.VMEM((4, 2, SIZE, SIZE), F32),
            pltpu.VMEM((10, 2, 64, 8, HALF), F32),
            pltpu.VMEM((2, 2, 8, 16, 8, HALF), F32),
            pltpu.VMEM((4, 2, 16, 8, HALF), F32),
            pltpu.VMEM((2, 2, 32, 8, HALF), F32),
            pltpu.VMEM((2, 2, 32, 8, HALF), F32),
            pltpu.VMEM((1, HALF), F32),
            pltpu.VMEM((3, 1, HALF), F32),
            pltpu.VMEM((1, HALF), F32),
            pltpu.VMEM((3, 1, HALF), F32),
            pltpu.VMEM((2, 1, HALF), F32),
            pltpu.VMEM((7, 2, 1, HALF), F32),
            pltpu.VMEM((2, 1, HALF), F32),
            pltpu.VMEM((1, 2, 1, HALF), F32),
            *chain_scratch(1),
            *chain_scratch(2),
            pltpu.SemaphoreType.DMA((152,)),
            pltpu.SemaphoreType.DMA((152,)),
            pltpu.SemaphoreType.DMA((18,)),
        ],
        compiler_params=pltpu.CompilerParams(
            collective_id=0, has_side_effects=True, vmem_limit_bytes=56 << 20
        ),
    )(
        positions, live_slots, object_slices.reshape(2, 32, 8, TC), probe_field, photon_counts[0, 0, 0],
        jnp.asarray(TABLE_HIGH), jnp.asarray(TABLE_LOW), jnp.asarray(TABLE_ORDER),
    )
    return (new_tile.reshape(1, 2, TR, TC), new_probe)


def solution(mesh):
    placed = (
        P("angle", None, "ty", "tx"),
        P(),
        P("angle", "ty", "tx", None, None),
        P("angle", "ty", "tx"),
        P("angle", "ty", "tx", None, None, None),
    )
    return jax.shard_map(
        body,
        mesh=mesh,
        in_specs=placed,
        out_specs=(P("angle", None, "ty", "tx"), P(None, "ty", None)),
        check_vma=False,
    )
```

```python
import functools
import math

import jax
import jax.numpy as jnp
import numpy as np
from jax import lax
from jax.experimental import pallas as pl
from jax.experimental.pallas import tpu as pltpu
from jax.sharding import PartitionSpec as P

MESH = pl.DeviceIdType.MESH
F32 = jnp.float32
BF16 = jnp.bfloat16
SIZE = 256
HALF = 128
TR = 256
TC = 1024
WR = TR + SIZE
WC = TC + SIZE
N_TY = 16
N_TX = 8
N_ANGLE = 2
N_XY = N_ANGLE * N_TX


def tables():
    n = np.arange(HALF)
    base = np.exp(-2j * np.pi * np.outer(n, n) / HALF) / 16.0
    odd = base * np.exp(-2j * np.pi * n / SIZE)[None, :]

    def real_form(m):
        return np.block([[m.real, -m.imag], [m.imag, m.real]])

    mats = [real_form(base), real_form(odd)]
    mats = np.stack([mats[0], mats[1], mats[0].T, mats[1].T]).astype(np.float32)
    high = mats.astype(jnp.bfloat16)
    low = (mats - high.astype(np.float32)).astype(jnp.bfloat16)
    order = np.zeros((SIZE, SIZE), np.float32)
    for j in range(SIZE):
        order[2 * j if j < HALF else 2 * (j - HALF) + 1, j] = 1.0
    both = np.stack([order, order.T]).astype(jnp.bfloat16)
    return high, low, both


TABLES = np.concatenate(tables())


def remote(src, dst, send, recv, **where):
    return pltpu.make_async_remote_copy(
        src_ref=src, dst_ref=dst, send_sem=send, recv_sem=recv, device_id=where, device_id_type=MESH
    )


def split(x):
    high = x.astype(BF16)
    return high, (x - high.astype(F32)).astype(BF16)


def dot(a, b):
    return jnp.dot(a, b, preferred_element_type=F32)


class Copies:
    def __init__(self, send, recv):
        self.send, self.recv, self.at = send, recv, 0

    def make(self, src, dst, **where):
        copy = remote(src, dst, self.send.at[self.at], self.recv.at[self.at], **where)
        self.at += 1
        return copy


def step_kernel(
    spots_s, live_s, tile, probe_h, counts_h, tables_h, new_tile, new_probe,
    wide, probe, counts, tables_v, around, around_s, power, padded, den, patches,
    canvas, vin, cin, hin, hout, pk_x, pk_x_in, pk_y, pk_y_in, pk, pk_z_in, pk_pair, pk_pair_in,
    den_sums, den_pair, den_mine, den_box, den_part, den_zbox, den_ybox, den_whole,
    num_sums, num_pair, num_mine, num_box, num_part, num_zbox, num_ybox, num_whole,
    send, recv, local,
):
    angle, ty, tx = lax.axis_index("angle"), lax.axis_index("ty"), lax.axis_index("tx")
    up, down = lax.rem(ty + N_TY - 1, N_TY), lax.rem(ty + 1, N_TY)
    left, right = lax.rem(tx + N_TX - 1, N_TX), lax.rem(tx + 1, N_TX)
    core, z = lax.rem(ty, 2), ty // 2
    x, y = tx // 2, 2 * angle + lax.rem(tx, 2)
    copies = Copies(send, recv)
    high, low, order = (tables_v.at[pl.ds(at, n)] for at, n in ((0, 4), (4, 4), (8, 2)))
    pair = {"ty": ty + 1 - 2 * core}

    def x_peer(step):
        other = lax.rem(x + step, 4)
        return other, {"tx": 2 * other + lax.rem(tx, 2)}

    def y_peer(step):
        other = lax.rem(y + step, 4)
        return other, {"angle": other // 2, "tx": 2 * x + lax.rem(other, 2)}

    def z_peer(step):
        other = lax.rem(z + step, 8)
        return other, {"ty": 2 * other + core}

    greeted = [{"tx": left}, {"tx": right}, {"ty": up}, {"ty": down}, pair]
    greeted += [x_peer(step)[1] for step in (1, 2, 3)] + [y_peer(step)[1] for step in (1, 2, 3)]
    greeted += [z_peer(step)[1] for step in range(1, 8)]
    barrier = pltpu.get_barrier_semaphore()
    for where in greeted:
        pl.semaphore_signal(barrier, inc=1, device_id=where, device_id_type=MESH)

    lane = lax.broadcasted_iota(jnp.int32, (1, HALF), 1)
    line = jnp.where(lane == 8, live_s[0, 0, 0], 0)
    for slot in range(4):
        for k in range(2):
            line = jnp.where(lane == 2 * slot + k, spots_s[0, 0, 0, slot, k], line)
    around[1, 1] = line

    middle_blocks, middle_groups = pl.ds(1, 8), pl.ds(16, 32)
    top_in, bottom_in = pl.ds(16, 16), pl.ds(32, 16)
    top_out, bottom_out = pl.ds(0, 16), pl.ds(48, 16)
    middle = [
        pltpu.make_async_copy(
            tile.at[:, :, :, pl.ds(block * HALF, HALF)], wide.at[1 + block, :, middle_groups], local.at[10 + block]
        )
        for block in range(8)
    ]
    loads = [
        pltpu.make_async_copy(src, dst, local.at[2 + k])
        for k, (src, dst) in enumerate(
            ((probe_h, probe), (tables_h, tables_v), (counts_h, counts))
        )
    ]
    for copy in middle:
        copy.start()
    loads[0].start()

    def clear(item, carry):
        padded[item // 16, lax.rem(item // 4, 4), lax.rem(item, 4)] = jnp.zeros((96, 8, HALF), F32)
        return carry

    lax.fori_loop(0, 32, clear, 0)
    lane32 = lax.broadcasted_iota(jnp.int32, (32, 8, HALF), 2)
    lane33 = lax.broadcasted_iota(jnp.int32, (33, 8, HALF), 2)
    sub32 = lax.broadcasted_iota(jnp.int32, (32, 8, HALF), 1)
    blank = jnp.zeros((1, 8, HALF), F32)

    def lay(channel, slot, by_row, by_col, x, part_rows=0, part_cols=0):
        count = 16 if part_rows else 32
        first = 16 if part_rows == -1 else 0
        inside = lax.broadcasted_iota(jnp.int32, (count, 8, HALF), 2) >= by_col
        below = lax.broadcasted_iota(jnp.int32, (count + 1, 8, HALF), 1) >= by_row

        def turned(part):
            part = part[8 * first : 8 * (first + count)].reshape(count, 8, HALF)
            return pltpu.roll(pltpu.roll(part, by_col, 2), by_row, 1)

        zero = jnp.zeros((count, 8, HALF), F32)
        one = zero if part_cols == -1 else turned(x[:, :HALF])
        two = zero if part_cols == 1 else turned(x[:, HALF:])
        parts = (
            None if part_cols == -1 else jnp.where(inside, one, zero),
            jnp.where(inside, two, one),
            None if part_cols == 1 else jnp.where(inside, zero, two),
        )
        for step, part in enumerate(parts):
            at = padded.at[channel, slot, 1 + step]
            if part is None:
                at[pl.ds(32, 33)] = jnp.zeros((33, 8, HALF), F32)
                continue
            moved = jnp.where(
                below, jnp.concatenate([part, blank], 0), jnp.concatenate([blank, part], 0)
            )
            at[pl.ds(32 + first, count + 1)] = moved
            if part_rows == 1:
                at[pl.ds(49, 16)] = jnp.zeros((16, 8, HALF), F32)
            if part_rows == -1:
                at[pl.ds(32, 16)] = jnp.zeros((16, 8, HALF), F32)

    def fetch(channel, spots, block, first, count, put):
        where = []
        for slot in range(4):
            at_group, at_block = spots[slot]
            near = block - at_block
            where.append((jnp.where((near >= 0) & (near <= 2), near + 1, 0), 32 + first - at_group))
        for step in range(count):
            total = None
            for slot, (index, start) in enumerate(where):
                part = padded[channel, slot, index, start + step]
                total = part if total is None else total + part
            put(step, total)

    def group(dy, dx, begin):
        spots = []
        for slot in range(4):
            if begin:
                row, col, used = spots_s[0, 0, 0, slot, 0], spots_s[0, 0, 0, slot, 1], slot < live_s[0, 0, 0]
            else:
                line = around_s.at[dy + 1, dx + 1, 0]
                row, col, used = line[2 * slot], line[2 * slot + 1], slot < line[8]
            row, col = row - ty * TR, col - tx * TC
            near = (row > -SIZE) & (row < TR) & (col > -SIZE) & (col < TC)
            weight = jnp.where(used & near, 1.0, 0.0).astype(F32)
            row = jnp.clip(row, -SIZE, TR - 1) + SIZE
            col = jnp.clip(col, -SIZE, TC - 1) + SIZE
            at_group, by_row = row // 8, lax.rem(row, 8)
            at_block, by_col = col // HALF, lax.rem(col, HALF)
            lay(0, slot, by_row, by_col, power[...] * weight, dy, dx)
            spots.append((at_group - 32, at_block - 2))
        first, count = {-1: (0, 16), 0: (0, 32), 1: (16, 16)}[dy]
        begin_block, end_block = {-1: (0, 1), 0: (0, 8), 1: (7, 8)}[dx]

        def one_block(block, carry):
            def put(step, total):
                if begin:
                    den[block, first + step] = total
                else:
                    den[block, first + step] += total

            fetch(0, spots, block, first, count, put)
            return carry

        lax.fori_loop(begin_block, end_block, one_block, 0)

    loads[0].wait()
    power[...] = probe[0] * probe[0] + probe[1] * probe[1]
    for copy in middle:
        copy.wait()
    pl.semaphore_wait(barrier, len(greeted))

    meta_sides = [
        copies.make(around.at[1, 1], around.at[1, 2], tx=left),
        copies.make(around.at[1, 1], around.at[1, 0], tx=right),
    ]
    sides = [
        [
            copies.make(wide.at[1, channel, middle_groups], wide.at[9, channel, middle_groups], tx=left),
            copies.make(wide.at[8, channel, middle_groups], wide.at[0, channel, middle_groups], tx=right),
        ]
        for channel in range(2)
    ]
    ends = [
        copies.make(wide.at[middle_blocks, :, top_in], wide.at[middle_blocks, :, bottom_out], ty=up),
        copies.make(wide.at[middle_blocks, :, bottom_in], wide.at[middle_blocks, :, top_out], ty=down),
    ]
    for copy in meta_sides + sides[0] + sides[1] + ends:
        copy.start()
    for load in loads[1:]:
        load.start()
    for copy in meta_sides:
        copy.wait()
    meta_ends = [
        copies.make(around.at[1], around.at[2], ty=up),
        copies.make(around.at[1], around.at[0], ty=down),
    ]
    for copy in meta_ends:
        copy.start()
    group(0, 0, True)
    for copy in meta_ends:
        copy.wait()
    scalars = pltpu.make_async_copy(around, around_s, local.at[7])
    scalars.start()
    scalars.wait()

    corners = []

    def relay(channel):
        for side, block in ((0, 0), (1, 9)):
            sides[channel][1 - side].wait_recv()
            for src, dst, where in ((top_in, bottom_out, {"ty": up}), (bottom_in, top_out, {"ty": down})):
                corners.append(copies.make(wide.at[block, channel, src], wide.at[block, channel, dst], **where))
                corners[-1].start()

    for dy, dx in ((-1, 0), (1, 0)):
        group(dy, dx, False)
    relay(0)
    for dy, dx in ((0, -1), (0, 1)):
        group(dy, dx, False)
    relay(1)
    for dy, dx in ((-1, -1), (-1, 1), (1, -1), (1, 1)):
        group(dy, dx, False)
    def share(value, own, others, peers):
        own[...] = value
        sent = [copies.make(own, others.at[k], **where) for k, where in enumerate(peers)]
        for copy in sent:
            copy.start()

        def finish():
            for copy in sent:
                copy.wait()
            top = own[...]
            for k in range(len(sent)):
                top = jnp.maximum(top, others[k])
            return top

        return finish

    top_x = share(
        jnp.broadcast_to(jnp.max(den[...]), (1, HALF)), pk_x, pk_x_in, [x_peer(step)[1] for step in (1, 2, 3)]
    )
    for side in sides[0] + sides[1]:
        side.wait_send()
    for copy in ends + corners:
        copy.wait()
    top_y = share(top_x(), pk_y, pk_y_in, [y_peer(step)[1] for step in (1, 2, 3)])

    den_sums[...] = jnp.zeros_like(den_sums)
    num_sums[...] = jnp.zeros_like(num_sums)

    def place_of(slot):
        row = jnp.clip(spots_s[0, 0, 0, slot, 0] - (ty * TR - HALF), 0, TR - 1)
        col = jnp.clip(spots_s[0, 0, 0, slot, 1] - (tx * TC - HALF), 0, TC - 1)
        return row // 8, lax.rem(row, 8), col // HALF, lax.rem(col, HALF)

    def weight_of(slot):
        return jnp.where(slot < live_s[0, 0, 0], 1.0, 0.0).astype(F32)

    def add_rows(sums, channel, value):
        value = value.reshape(8, 2, 2, 8, SIZE)
        for parity in range(2):
            for quarter in range(4):
                side = HALF * (quarter % 2)
                sums[parity, quarter, :, channel] += value[:, parity, quarter // 2, :, side : side + HALF]

    def cut(slot, carry):
        at_group, by_row, at_block, by_col = place_of(slot)
        back_row, back_col = lax.rem(8 - by_row, 8), lax.rem(HALF - by_col, HALF)
        square = None
        for channel in range(2):
            parts = []
            for step in range(3):
                x = jnp.stack([wide[at_block + step, channel, at_group + k] for k in range(33)])
                parts.append(pltpu.roll(x, back_col, 2))
            done = []
            for step in range(2):
                x = jnp.where(lane33 < HALF - by_col, parts[step], parts[step + 1])
                x = pltpu.roll(x, back_row, 1)
                x = jnp.where(sub32 < 8 - by_row, x[:32], x[1:])
                done.append(x.reshape(SIZE, HALF))
            x = jnp.concatenate(done, 1)
            patches[slot, channel] = x
            square = x * x if square is None else square + x * x
        add_rows(den_sums, 0, square * weight_of(slot))
        return carry

    lax.fori_loop(0, 4, cut, 0)

    class Chain:
        def __init__(self, sums, pair_in, mine, box, part, zbox, ybox, whole):
            self.__dict__.update(sums=sums, pair_in=pair_in, mine=mine, box=box, part=part, zbox=zbox, ybox=ybox, whole=whole)
            self.over_pair = copies.make(sums.at[1 - core], pair_in, **pair)
            self.over_x = [
                copies.make(mine.at[x_peer(step)[0]], box.at[step], **x_peer(step)[1]) for step in (1, 2, 3)
            ]
            self.over_z = [
                copies.make(part.at[z_peer(step)[0]], zbox.at[step], **z_peer(step)[1]) for step in range(1, 8)
            ]
            self.over_y = [copies.make(ybox.at[y], ybox.at[y], **y_peer(step)[1]) for step in (1, 2, 3)]
            self.out = [copies.make(whole.at[x], whole.at[x], **x_peer(step)[1]) for step in (1, 2, 3)]

        def start_pair(self):
            self.over_pair.start()

        def start_x(self):
            self.over_pair.wait()
            self.mine[...] = self.sums[core] + self.pair_in[...]
            for copy in self.over_x:
                copy.start()

        def start_z(self):
            for copy in self.over_x:
                copy.wait()
            self.part[...] = self.mine[x] + self.box[1] + self.box[2] + self.box[3]
            for copy in self.over_z:
                copy.start()

        def start_y(self):
            for copy in self.over_z:
                copy.wait()
            total = self.part[z]
            for step in range(1, 8):
                total = total + self.zbox[step]
            self.ybox[y] = total
            for copy in self.over_y:
                copy.start()

        def start_out(self):
            for copy in self.over_y:
                copy.wait()
            self.whole[x] = (self.ybox[0] + self.ybox[1]) + (self.ybox[2] + self.ybox[3])
            for copy in self.out:
                copy.start()

        def finish(self):
            for copy in self.out:
                copy.wait()

    den_chain = Chain(den_sums, den_pair, den_mine, den_box, den_part, den_zbox, den_ybox, den_whole)
    num_chain = Chain(num_sums, num_pair, num_mine, num_box, num_part, num_zbox, num_ybox, num_whole)
    den_chain.start_pair()
    for load in loads[1:]:
        load.wait()

    def from_left(which, x):
        a, b = split(x)
        return dot(high[which], a) + (dot(high[which], b) + dot(low[which], a))

    def from_right(x, which):
        a, b = split(x)
        return dot(a, high[which]) + (dot(b, high[which]) + dot(a, low[which]))

    def one_slot(slot, carry):
        at_group, by_row, at_block, by_col = place_of(slot)
        weight = weight_of(slot)
        xr, xi = patches[slot, 0], patches[slot, 1]
        qr, qi = probe[0], probe[1]
        pr, pi = qr * xr - qi * xi, qr * xi + qi * xr
        even = from_right(
            jnp.concatenate([pr[:, :HALF] + pr[:, HALF:], pi[:, :HALF] + pi[:, HALF:]], 1), 2
        )
        odd = from_right(
            jnp.concatenate([pr[:, :HALF] - pr[:, HALF:], pi[:, :HALF] - pi[:, HALF:]], 1), 3
        )
        mr = jnp.concatenate([even[:, :HALF], odd[:, :HALF]], 1)
        mi = jnp.concatenate([even[:, HALF:], odd[:, HALF:]], 1)
        fe = from_left(0, jnp.concatenate([mr[:HALF] + mr[HALF:], mi[:HALF] + mi[HALF:]], 0))
        fo = from_left(1, jnp.concatenate([mr[:HALF] - mr[HALF:], mi[:HALF] - mi[HALF:]], 0))
        count = counts[slot]
        tens = lax.shift_right_logical(count, 4)
        ones = count - 16 * tens
        tens = dot(dot(order[1], tens.astype(F32).astype(BF16)).astype(BF16), order[0])
        ones = dot(dot(order[1], ones.astype(F32).astype(BF16)).astype(BF16), order[0])
        count = 16.0 * tens + ones

        def scaled(f, c):
            re, im = f[:HALF], f[HALF:]
            size = jnp.maximum(re * re + im * im, 0.0625)
            factor = (0.05 * c) * lax.rsqrt(c * size)
            return jnp.concatenate([re * factor, im * factor], 0)

        ge = from_left(2, scaled(fe, count[:HALF]))
        go = from_left(3, scaled(fo, count[HALF:]))
        top, bottom = ge + go, ge - go
        hr_ = jnp.concatenate([top[:HALF], bottom[:HALF]], 0)
        hi_ = jnp.concatenate([top[HALF:], bottom[HALF:]], 0)
        be = from_right(jnp.concatenate([hr_[:, :HALF], hi_[:, :HALF]], 1), 0)
        bo = from_right(jnp.concatenate([hr_[:, HALF:], hi_[:, HALF:]], 1), 1)
        first, second = be + bo, be - bo
        dr = (jnp.concatenate([first[:, :HALF], second[:, :HALF]], 1) - pr) * weight
        di = (jnp.concatenate([first[:, HALF:], second[:, HALF:]], 1) - pi) * weight
        lay(0, slot, by_row, by_col, qr * dr + qi * di)
        lay(1, slot, by_row, by_col, qr * di - qi * dr)
        add_rows(num_sums, 0, xr * dr + xi * di)
        add_rows(num_sums, 1, xr * di - xi * dr)
        return carry

    one_slot(0, 0)
    den_chain.start_x()
    one_slot(1, 0)
    one_slot(2, 0)
    den_chain.start_z()
    one_slot(3, 0)
    num_chain.start_pair()

    places = [(place_of(slot)[0], place_of(slot)[2]) for slot in range(4)]

    def one_canvas(first, count):
        def add(block, carry):
            for channel in range(2):
                def put(step, total):
                    canvas[block, channel, first + step] = total

                fetch(channel, places, block, first, count, put)
            return carry

        return add

    lax.fori_loop(0, 2, lambda k, carry: one_canvas(0, 64)(9 * k, carry), 0)
    back_corners = []
    for side, block in ((0, 0), (1, 9)):
        for way, (src, where) in enumerate(((top_out, {"ty": up}), (bottom_out, {"ty": down}))):
            back_corners.append(copies.make(canvas.at[block, :, src], cin.at[2 * side + way], **where))
            back_corners[-1].start()
    num_chain.start_x()
    den_chain.start_y()
    lax.fori_loop(1, 9, one_canvas(0, 16), 0)
    lax.fori_loop(1, 9, one_canvas(48, 16), 0)
    back_ends = []
    for channel in range(2):
        for part in range(2):
            blocks, there = pl.ds(1 + 4 * part, 4), pl.ds(4 * part, 4)
            back_ends.append(
                [
                    copies.make(canvas.at[blocks, channel, top_out], vin.at[0, channel, there], ty=up),
                    copies.make(canvas.at[blocks, channel, bottom_out], vin.at[1, channel, there], ty=down),
                ]
            )

    def start_ends(k):
        for copy in back_ends[k]:
            copy.start()

    start_ends(0)
    den_chain.start_out()
    for copy in back_corners:
        copy.wait()
    for side, block in ((0, 0), (1, 9)):
        hout[side, :, pl.ds(0, 16)] = canvas[block, :, top_in] + cin[2 * side + 1]
        hout[side, :, pl.ds(16, 16)] = canvas[block, :, bottom_in] + cin[2 * side]
    across = [
        copies.make(hout.at[0], hin.at[0], tx=left),
        copies.make(hout.at[1], hin.at[1], tx=right),
    ]
    for copy in across:
        copy.start()
    start_ends(1)
    num_chain.start_z()
    den_chain.finish()
    pk[0] = top_y()
    pk[1] = jnp.broadcast_to(jnp.max(den_whole[...]), (1, HALF))
    top_z = share(pk[...], pk, pk_z_in, [z_peer(step)[1] for step in range(1, 8)])
    start_ends(2)
    lax.fori_loop(1, 9, one_canvas(16, 32), 0)
    num_chain.start_y()
    start_ends(3)
    top_pair = share(top_z(), pk_pair, pk_pair_in, [pair])
    num_chain.start_out()
    top = top_pair()
    peak_obj, peak_probe = top[0, 0, 0], top[1, 0, 0]
    den[...] = 1.0 / (den[...] + 0.1 * peak_obj)
    for copy in [copy for both in back_ends for copy in both]:
        copy.wait()

    def update(block):
        for channel in range(2):
            for first, side in ((0, 1), (16, 0)):
                here, there = pl.ds(16 + first, 16), pl.ds(first, 16)
                value = canvas[1 + block, channel, here] + vin[side, channel, block]
                new_tile[channel, there, :, pl.ds(block * HALF, HALF)] = (
                    wide[1 + block, channel, here] + value * den[block, there]
                )

    for block in range(1, 7):
        update(block)
    for copy in across:
        copy.wait()
    for block, side in ((7, 0), (0, 1)):
        canvas[1 + block, :, middle_groups] += hin[side]
        update(block)
    num_chain.finish()
    for quarter in range(4):
        rows = pl.ds(pl.multiple_of(16 * ty + 8 * (quarter // 2), 8), 8)
        cols = pl.ds(HALF * (quarter % 2), HALF)
        scale = 1.0 / (den_whole[quarter, 0] + 0.1 * peak_probe)
        for channel in range(2):
            new_probe[channel, pl.ds(8 * (quarter // 2), 8), cols] = (
                probe[channel, rows, cols] + num_whole[quarter, channel] * scale
            )


def vmem():
    return pl.BlockSpec(memory_space=pltpu.VMEM)


def chain_scratch(channels):
    piece = (channels, 8, HALF)
    shapes = (
        (2, 4, 8) + piece, (4, 8) + piece, (4, 8) + piece, (4, 8) + piece,
        (8,) + piece, (8,) + piece, (4,) + piece, (4,) + piece,
    )
    return [pltpu.VMEM(shape, F32) for shape in shapes]


def body(object_slices, probe_field, positions, live_slots, photon_counts):
    new_tile, new_probe = pl.pallas_call(
        step_kernel,
        name="step",
        out_shape=(
            jax.ShapeDtypeStruct((2, 32, 8, TC), F32),
            jax.ShapeDtypeStruct((2, 16, SIZE), F32),
        ),
        in_specs=[pl.BlockSpec(memory_space=pltpu.SMEM)] * 2 + [pl.BlockSpec(memory_space=pltpu.HBM)] * 4,
        out_specs=(vmem(), vmem()),
        scratch_shapes=[
            pltpu.VMEM((10, 2, 64, 8, HALF), F32),
            pltpu.VMEM((2, SIZE, SIZE), F32),
            pltpu.VMEM((4, SIZE, SIZE), jnp.int32),
            pltpu.VMEM((10, SIZE, SIZE), BF16),
            pltpu.VMEM((3, 3, 1, HALF), jnp.int32),
            pltpu.SMEM((3, 3, 1, HALF), jnp.int32),
            pltpu.VMEM((SIZE, SIZE), F32),
            pltpu.VMEM((2, 4, 4, 96, 8, HALF), F32),
            pltpu.VMEM((8, 32, 8, HALF), F32),
            pltpu.VMEM((4, 2, SIZE, SIZE), F32),
            pltpu.VMEM((10, 2, 64, 8, HALF), F32),
            pltpu.VMEM((2, 2, 8, 16, 8, HALF), F32),
            pltpu.VMEM((4, 2, 16, 8, HALF), F32),
            pltpu.VMEM((2, 2, 32, 8, HALF), F32),
            pltpu.VMEM((2, 2, 32, 8, HALF), F32),
            pltpu.VMEM((1, HALF), F32),
            pltpu.VMEM((3, 1, HALF), F32),
            pltpu.VMEM((1, HALF), F32),
            pltpu.VMEM((3, 1, HALF), F32),
            pltpu.VMEM((2, 1, HALF), F32),
            pltpu.VMEM((7, 2, 1, HALF), F32),
            pltpu.VMEM((2, 1, HALF), F32),
            pltpu.VMEM((1, 2, 1, HALF), F32),
            *chain_scratch(1),
            *chain_scratch(2),
            pltpu.SemaphoreType.DMA((152,)),
            pltpu.SemaphoreType.DMA((152,)),
            pltpu.SemaphoreType.DMA((18,)),
        ],
        compiler_params=pltpu.CompilerParams(
            collective_id=0, has_side_effects=True, vmem_limit_bytes=48 << 20
        ),
    )(
        positions, live_slots, object_slices.reshape(2, 32, 8, TC), probe_field, photon_counts[0, 0, 0],
        jnp.asarray(TABLES),
    )
    return (new_tile.reshape(1, 2, TR, TC), new_probe)


def solution(mesh):
    placed = (
        P("angle", None, "ty", "tx"),
        P(),
        P("angle", "ty", "tx", None, None),
        P("angle", "ty", "tx"),
        P("angle", "ty", "tx", None, None, None),
    )
    return jax.shard_map(
        body,
        mesh=mesh,
        in_specs=placed,
        out_specs=(P("angle", None, "ty", "tx"), P(None, "ty", None)),
        check_vma=False,
    )
```
